512 devices in a mesh: section: 8 (over y, core), shard: 64 (over x, z).
Axes of the slice: x: 4, y: 4, z: 16, core: 2. Of those that a mesh axis runs over, the one named last changes fastest.
Arguments:
- section_input: bfloat16 [4, 64, 196, 256], P(None, 'shard'), may hold values from -6 to 6
- conv_one: bfloat16 [8, 2304, 256], P('section'), may hold values from -0.125 to 0.125
- conv_two: bfloat16 [8, 2304, 256], P('section'), may hold values from -0.125 to 0.125
- unit_gain: float32 [8, 256], P('section'), may hold values from 0.5 to 1.5
- offset_bias: float32 [8, 256], P('section'), may hold values from -3 to 3
- leak_slope: float32 [8, 256], P('section'), may hold values from 0.1 to 0.4
- depthwise: bfloat16 [196, 256], replicated, may hold values from -0.4375 to 0.4375
- embed_weight: bfloat16 [256, 512], replicated, may hold values from -0.375 to 0.375
- class_centers: bfloat16 [106496, 512], P('shard'), may hold values from -6 to 6
- labels: int32 [4, 64], replicated, may hold values from 0 to 106495
- class_offsets: int32 [64], P('shard'), may hold values from 0 to 104832, as said below
Outputs:
- section_grads: bfloat16 [8, 4, 64, 196, 256], P('section', None, 'shard')
The draws below stay inside these ranges and needn't reach their ends.
Inputs may be any that keep to these rules, and one draw needn't show every extreme that they name: `class_offsets`: each entry is 1664 times a different number of 0 to 63, so the blocks of class_centers hold every class of 0 to 106495 once.
All inputs are finite; a program needn't handle non-finite values.
Results may differ from the reference program's by a relative error of at most 0.03.
Values may be sent and summed in bfloat16 or wider, within the bound.
No kernel may reach another device: no remote copies, remote signals or barrier semaphores. Data moves between devices by JAX's collectives and lax.ppermute only.
A program may use at most 64 MiB of HBM per device.

```python
import math
import jax
import jax.numpy as jnp
from jax import lax

C = 256
EMB = 512
SIDE = 14
CLS_DEV = 1664
MICRO = 4
FACES = 64
CLASSES = 106496
N_SECTION = 8
N_SHARD = 64


def draw_class_offsets(key, part):
    order = jax.random.permutation(jax.random.fold_in(key, 17), N_SHARD)
    return (order * CLS_DEV).astype(jnp.int32)


def plant(entries, own_key, low, top_value):
    longest = entries.shape.index(max(entries.shape))
    spots = []
    for shift in (0, 1):
        where = [jax.random.randint(jax.random.fold_in(own_key, axis), (), 0, length) for axis, length in enumerate(entries.shape)]
        where[longest] = (where[longest] + shift) % entries.shape[longest]
        spots.append(tuple(where))
    return entries.at[spots[0]].set(low).at[spots[1]].set(top_value)


def levels(own_key, extent, cuts, low, largest):
    def one(position, shards_of):
        draws = jax.random.uniform(jax.random.fold_in(jax.random.fold_in(own_key, 6), position), (shards_of,), jnp.float32, low / len(cuts), largest / len(cuts))
        return jnp.repeat(jnp.exp(draws), extent[position] // shards_of).reshape((-1,) + (1,) * (len(extent) - position - 1))

    gain = one(*cuts[0])
    for cut in cuts[1:]:
        gain = gain * one(*cut)
    return gain


def scatter_about(stream_key, extent, deviation, most, split=(), kind=jnp.bfloat16):
    factor_of = levels(stream_key, extent, split, -0.22, 0.18) if split else 1.0
    values = jax.random.normal(stream_key, extent, jnp.float32) * deviation * factor_of
    return jnp.minimum(jnp.maximum(values, -most), most).astype(kind)


def setup_inputs(seed: int = 0) -> dict:
    key_of = jax.random.split(jax.random.key(seed), 12)
    return {
        "section_input": scatter_about(key_of[0], (MICRO, FACES, SIDE * SIDE, C), 1.0, 6.0, ((1, 64),)),
        "conv_one": scatter_about(key_of[1], (N_SECTION, 9 * C, C), (9 * C) ** -0.5, 0.125, ((0, 8),)),
        "conv_two": scatter_about(key_of[2], (N_SECTION, 9 * C, C), (9 * C) ** -0.5, 0.125, ((0, 8),)),
        "unit_gain": jnp.clip(1.0 + 0.1 * jax.random.normal(key_of[3], (N_SECTION, C), jnp.float32), 0.5, 1.5),
        "offset_bias": scatter_about(key_of[4], (N_SECTION, C), 0.5, 3.0, ((0, 8),), jnp.float32),
        "leak_slope": jnp.clip(0.1 + 0.3 * jax.random.uniform(key_of[5], (N_SECTION, C), jnp.float32) ** levels(key_of[5], (N_SECTION, C), ((0, 8),), -0.2, 0.2), 0.1, 0.4),
        "depthwise": scatter_about(key_of[6], (SIDE * SIDE, C), (SIDE * SIDE) ** -0.5, 0.4375),
        "embed_weight": scatter_about(key_of[7], (C, EMB), C ** -0.5, 0.375),
        "class_centers": scatter_about(key_of[8], (CLASSES, EMB), 1.0, 6.0, ((0, 64),)),
        "labels": plant(jax.random.randint(key_of[9], (MICRO, FACES), 0, CLASSES), jax.random.fold_in(key_of[9], 1), 0, CLASSES - 1).astype(jnp.int32),
        "class_offsets": draw_class_offsets(jax.random.fold_in(key_of[11], 71), 0),
    }


margin_value = 0.4
scale_value = 64.0
tiny_value = 1e-06

def conv_apply(images, weights):
    image_count = images.shape[0]
    channels = images.shape[-1]
    image_grid = images.reshape(image_count, SIDE, SIDE, channels)
    padded = jnp.pad(image_grid, ((0, 0), (1, 1), (1, 1), (0, 0)))
    pieces = [padded[:, row_shift:row_shift + SIDE, col_shift:col_shift + SIDE, :] for row_shift in range(3) for col_shift in range(3)]
    columns = jnp.concatenate(pieces, axis=3).reshape(image_count * SIDE * SIDE, 9 * channels)
    result = jnp.dot(columns, weights, preferred_element_type=jnp.float32)
    return result.reshape(image_count, SIDE * SIDE, weights.shape[1])

def flip_weights(weights):
    channels = weights.shape[1]
    tap_blocks = weights.reshape(9, channels, channels)
    return jnp.swapaxes(tap_blocks[::-1], 1, 2).reshape(9 * channels, channels)

def smooth_active(pre_active, leak):
    return leak * pre_active + (1.0 - leak) * jax.nn.softplus(4.0 * pre_active) / 4.0

def smooth_slope(pre_active, leak):
    return leak + (1.0 - leak) * jax.nn.sigmoid(4.0 * pre_active)

def unit_forward(images, first_weight, second_weight, gain_row, bias_row, leak_row):
    hidden = conv_apply(images, first_weight)
    pre_active = hidden * gain_row + bias_row
    active = smooth_active(pre_active, leak_row).astype(jnp.bfloat16)
    output = (images.astype(jnp.float32) + conv_apply(active, second_weight)).astype(jnp.bfloat16)
    return (output, pre_active)

def unit_backward(grad_out, pre_active, first_flip, second_flip, gain_row, leak_row):
    grad_active = conv_apply(grad_out, second_flip)
    grad_hidden = (grad_active * smooth_slope(pre_active, leak_row) * gain_row).astype(jnp.bfloat16)
    return (grad_out.astype(jnp.float32) + conv_apply(grad_hidden, first_flip)).astype(jnp.bfloat16)

def unit_scale(values):
    squares = lax.optimization_barrier(jnp.mean(values * values, axis=-1, keepdims=True))
    factor = lax.rsqrt(squares + tiny_value) / math.sqrt(values.shape[-1])
    return (values * factor, squares, factor)

def reference(section_input, conv_one, conv_two, unit_gain, offset_bias, leak_slope, depthwise, embed_weight, class_centers, labels, class_offsets):
    row_count = MICRO * FACES
    current = section_input.reshape(row_count, SIDE * SIDE, C)
    pre_list = []
    for section_index in range(N_SECTION):
        current, pre_active = unit_forward(current, conv_one[section_index], conv_two[section_index], unit_gain[section_index], offset_bias[section_index], leak_slope[section_index])
        pre_list.append(pre_active)
    pooled = jnp.einsum('rpc,pc->rc', current.astype(jnp.float32), depthwise.astype(jnp.float32)).astype(jnp.bfloat16)
    embedded = jnp.dot(pooled, embed_weight, preferred_element_type=jnp.float32)
    normed, squares, factor = unit_scale(embedded)
    unit_half = normed.astype(jnp.bfloat16)
    flat_labels = labels.reshape(row_count)
    blocks = class_centers.reshape(N_SHARD, CLS_DEV, EMB)

    def one_block(running, inputs):
        center_block, class_base = inputs
        centres_unit = unit_scale(center_block.astype(jnp.float32))[0].astype(jnp.bfloat16)
        cosines = jnp.dot(unit_half, centres_unit.T, preferred_element_type=jnp.float32)
        class_ids = class_base + jnp.arange(CLS_DEV, dtype=jnp.int32)
        label_hits = flat_labels[:, None] == class_ids[None, :]
        logits = scale_value * (cosines - margin_value * label_hits.astype(jnp.float32))
        exp_logits = jnp.exp(logits)
        weighted = jnp.dot(exp_logits.astype(jnp.bfloat16), centres_unit, preferred_element_type=jnp.float32)
        chosen = jnp.dot(label_hits.astype(jnp.bfloat16), centres_unit, preferred_element_type=jnp.float32)
        return ((running[0] + weighted, running[1] + chosen, running[2] + lax.optimization_barrier(jnp.sum(exp_logits, axis=1))), None)
    start_sums = (jnp.zeros((row_count, EMB), jnp.float32), jnp.zeros((row_count, EMB), jnp.float32), jnp.zeros((row_count,), jnp.float32))
    sums_out = lax.scan(one_block, start_sums, (blocks, class_offsets.astype(jnp.int32)))[0]
    grad_unit = scale_value * (sums_out[0] / sums_out[2][:, None] - sums_out[1])
    inner = lax.optimization_barrier(jnp.sum(embedded * grad_unit, axis=-1, keepdims=True))
    grad_embed = factor * (grad_unit - embedded * inner / (EMB * (squares + tiny_value)))
    grad_pooled = jnp.dot(grad_embed.astype(jnp.bfloat16), embed_weight.T, preferred_element_type=jnp.float32)
    current_grad = (grad_pooled[:, None, :] * depthwise.astype(jnp.float32)[None, :, :]).astype(jnp.bfloat16)
    grad_list = [None] * N_SECTION
    for section_index in reversed(range(N_SECTION)):
        current_grad = unit_backward(current_grad, pre_list[section_index], flip_weights(conv_one[section_index]), flip_weights(conv_two[section_index]), unit_gain[section_index], leak_slope[section_index])
        grad_list[section_index] = current_grad
    return jnp.stack(grad_list).reshape(N_SECTION, MICRO, FACES, SIDE * SIDE, C)
```

```python
import functools
import math

import jax
import jax.numpy as jnp
from jax import lax
from jax.experimental import pallas as pl
from jax.experimental.pallas import tpu as pltpu
from jax.sharding import PartitionSpec as P

SIDE = 14
WIDE = 16
ROWS = SIDE * WIDE
C = 256

margin_value = 0.4
scale_value = 64.0
tiny_value = 1e-06

VM = pl.BlockSpec(memory_space=pltpu.VMEM)
SM = pl.BlockSpec(memory_space=pltpu.SMEM)
LIMIT = 20 * 1024 * 1024


def in_vmem(x):
    return pltpu.with_memory_space_constraint(x, pltpu.VMEM)


def keep_columns(rows):
    return (lax.broadcasted_iota(jnp.int32, (rows, C), 0) % WIDE) < SIDE


def clear_border(cols):
    zero = jnp.zeros((cols.shape[0], WIDE, cols.shape[2]), cols.dtype)
    cols[:, 0:WIDE, :] = zero
    cols[:, WIDE + ROWS : 2 * WIDE + ROWS, :] = zero


def conv(value, weights, cols):
    images = cols.shape[0]
    total = images * ROWS
    before = pltpu.roll(value, 1, 0)
    after = pltpu.roll(value, total - 1, 0)
    for place, part in enumerate((before, value, after)):
        cols[:, WIDE : WIDE + ROWS, place * C : (place + 1) * C] = part.astype(jnp.bfloat16).reshape(
            images, ROWS, C
        )
    acc = None
    for step in range(3):
        left = cols[:, WIDE * step : WIDE * step + ROWS, :].reshape(total, 3 * C)
        part = jnp.dot(
            left, weights[step * 3 * C : (step + 1) * 3 * C, :], preferred_element_type=jnp.float32
        )
        acc = part if acc is None else acc + part
    return acc


def forward_body(flag, x_ref, w1_ref, w2_ref, vec_ref, z_in, out_ref, z_ref, cols, run):
    images = cols.shape[0]
    total = images * ROWS

    @pl.when(flag[0] == 1)
    def _():
        clear_border(cols)
        keep = keep_columns(total)
        run[...] = x_ref[...].astype(jnp.float32).reshape(total, C)

        def one(u, carry):
            value = run[...]
            hidden = conv(value, w1_ref.at[u], cols)
            vec = vec_ref[u]
            pre = hidden * vec[0:1] + vec[1:2]
            z_ref[u] = pre
            leak = vec[2:3]
            four = 4.0 * pre
            soft = jnp.maximum(four, 0.0) + jnp.log1p(jnp.exp(-jnp.abs(four)))
            active = leak * pre + (1.0 - leak) * soft * 0.25
            active = jnp.where(keep, active, 0.0)
            result = run[...] + conv(active, w2_ref.at[u], cols)
            result = jnp.where(keep, result, 0.0).astype(jnp.bfloat16)
            run[...] = result.astype(jnp.float32)
            return carry

        lax.fori_loop(0, 2, one, 0)
        out_ref[...] = run[...].astype(jnp.bfloat16).reshape(images, ROWS, C)


def backward_body(flag, g_ref, f1_ref, f2_ref, vec_ref, z_ref, store_in, out_ref, store, cols, run):
    images = cols.shape[0]
    total = images * ROWS

    @pl.when(flag[0] == 1)
    def _():
        clear_border(cols)
        keep = keep_columns(total)
        run[...] = g_ref[...].astype(jnp.float32).reshape(total, C)

        def one(step, carry):
            u = 1 - step
            grad_active = conv(run[...], f2_ref.at[u], cols)
            vec = vec_ref[u]
            pre = z_ref[u]
            leak = vec[2:3]
            slope = leak + (1.0 - leak) / (1.0 + jnp.exp(-4.0 * pre))
            grad_hidden = jnp.where(keep, grad_active * slope * vec[0:1], 0.0)
            result = run[...] + conv(grad_hidden, f1_ref.at[u], cols)
            result = jnp.where(keep, result, 0.0).astype(jnp.bfloat16)
            run[...] = result.astype(jnp.float32)
            store[u] = result.reshape(images, ROWS, C)
            return carry

        lax.fori_loop(0, 2, one, 0)
        out_ref[...] = run[...].astype(jnp.bfloat16).reshape(images, ROWS, C)


CONV_COST = pl.CostEstimate(flops=4 * 2 * 448 * 2304 * 256, bytes_accessed=6_000_000, transcendentals=500_000)


def forward_stage(flag, x, w1, w2, vec, z):
    images = x.shape[0]
    return pl.pallas_call(
        forward_body,
        in_specs=[SM, VM, VM, VM, VM, VM],
        out_specs=[VM, VM],
        out_shape=[jax.ShapeDtypeStruct(x.shape, jnp.bfloat16), jax.ShapeDtypeStruct(z.shape, z.dtype)],
        scratch_shapes=[
            pltpu.VMEM((images, ROWS + 2 * WIDE, 3 * C), jnp.bfloat16),
            pltpu.VMEM((images * ROWS, C), jnp.float32),
        ],
        input_output_aliases={5: 1},
        compiler_params=pltpu.CompilerParams(vmem_limit_bytes=LIMIT),
        cost_estimate=CONV_COST,
        name="forward_stage",
    )(flag, in_vmem(x), in_vmem(w1), in_vmem(w2), in_vmem(vec), in_vmem(z))


def backward_stage(flag, g, f1, f2, vec, z, store):
    images = g.shape[0]
    return pl.pallas_call(
        backward_body,
        in_specs=[SM, VM, VM, VM, VM, VM, VM],
        out_specs=[VM, VM],
        out_shape=[
            jax.ShapeDtypeStruct(g.shape, jnp.bfloat16),
            jax.ShapeDtypeStruct(store.shape, store.dtype),
        ],
        scratch_shapes=[
            pltpu.VMEM((images, ROWS + 2 * WIDE, 3 * C), jnp.bfloat16),
            pltpu.VMEM((images * ROWS, C), jnp.float32),
        ],
        input_output_aliases={6: 1},
        compiler_params=pltpu.CompilerParams(vmem_limit_bytes=LIMIT),
        cost_estimate=CONV_COST,
        name="backward_stage",
    )(flag, in_vmem(g), in_vmem(f1), in_vmem(f2), in_vmem(vec), in_vmem(z), in_vmem(store))


def flip_body(w1_ref, w2_ref, f1_ref, f2_ref):
    eye = (
        lax.broadcasted_iota(jnp.int32, (C, C), 0) == lax.broadcasted_iota(jnp.int32, (C, C), 1)
    ).astype(jnp.float32).astype(jnp.bfloat16)
    for source, target in ((w1_ref, f1_ref), (w2_ref, f2_ref)):

        def one(u, carry):
            for tap in range(9):
                block = source[u, tap * C : (tap + 1) * C, :]
                turned = lax.dot_general(
                    eye, block, (((1,), (1,)), ((), ())), preferred_element_type=jnp.float32
                )
                target[u, (8 - tap) * C : (9 - tap) * C, :] = turned.astype(jnp.bfloat16)
            return carry

        lax.fori_loop(0, 2, one, 0)


def flip_all(w1, w2):
    return pl.pallas_call(
        flip_body,
        in_specs=[VM, VM],
        out_specs=[VM, VM],
        out_shape=[jax.ShapeDtypeStruct(w1.shape, w1.dtype)] * 2,
        compiler_params=pltpu.CompilerParams(vmem_limit_bytes=LIMIT),
        cost_estimate=pl.CostEstimate(flops=36 * 2 * 256**3, bytes_accessed=9_000_000, transcendentals=0),
        name="flip_all",
    )(in_vmem(w1), in_vmem(w2))


def unit_scale(values):
    squares = jnp.mean(values * values, axis=-1, keepdims=True)
    factor = lax.rsqrt(squares + tiny_value) / math.sqrt(values.shape[-1])
    return (values * factor, squares, factor)


def on_device(
    section_input,
    conv_one,
    conv_two,
    unit_gain,
    offset_bias,
    leak_slope,
    depthwise,
    embed_weight,
    class_centers,
    labels,
    class_offsets,
):
    sections = lax.axis_size("section")
    shards = lax.axis_size("shard")
    planes = sections // 2
    section_index = lax.axis_index("section")
    plane = section_index // 2
    core = section_index % 2
    swap = [(s, s ^ 1) for s in range(sections)]

    def stacked(own):
        peer = lax.ppermute(own, "section", swap)
        both = jnp.zeros((2, *own.shape), own.dtype)
        both = lax.dynamic_update_index_in_dim(both, own, core, 0)
        return lax.dynamic_update_index_in_dim(both, peer, 1 - core, 0)

    vec = stacked(jnp.concatenate([unit_gain, offset_bias, leak_slope], axis=0))
    w1 = stacked(conv_one[0])
    w2 = stacked(conv_two[0])
    micro = section_input.shape[0] // 2

    def widened(rows):
        grid = rows.reshape(-1, SIDE, SIDE, C)
        return jnp.pad(grid, ((0, 0), (0, 0), (0, WIDE - SIDE), (0, 0))).reshape(-1, ROWS, C)

    mine = lax.dynamic_slice_in_dim(section_input[:, 0], core * micro, micro, 0)
    x = widened(mine)
    pool_weight = widened(depthwise)[0].astype(jnp.float32)
    z = jnp.zeros((2, micro * ROWS, C), jnp.float32)
    flags = [(plane == s).astype(jnp.int32).reshape(1) for s in range(planes)]

    f1 = f2 = None
    for s in range(planes):
        x, z = forward_stage(flags[s], x, w1, w2, vec, z)
        if s == 0:
            f1, f2 = flip_all(w1, w2)
        if s < planes - 1:
            x = lax.ppermute(x, "section", [(2 * s + c, 2 * s + 2 + c) for c in range(2)])

    pooled = jnp.sum(x.astype(jnp.float32) * pool_weight[None], axis=1).astype(jnp.bfloat16)
    embedded = jnp.dot(pooled, embed_weight, preferred_element_type=jnp.float32)
    normed, squares, factor = unit_scale(embedded)
    sent = jnp.broadcast_to(normed.astype(jnp.bfloat16)[None], (shards, *normed.shape))
    unit_half = lax.all_to_all(sent, "shard", 0, 0, tiled=True).reshape(shards * micro, -1)
    centres_unit = unit_scale(class_centers.astype(jnp.float32))[0].astype(jnp.bfloat16)
    class_ids = class_offsets[0] + jnp.arange(class_centers.shape[0], dtype=jnp.int32)
    my_labels = lax.dynamic_slice_in_dim(labels, core * micro, micro, 0).T.reshape(-1)
    label_hits = my_labels[:, None] == class_ids[None, :]
    cosines = lax.dot_general(
        unit_half, centres_unit, (((1,), (1,)), ((), ())), preferred_element_type=jnp.float32
    )
    logits = scale_value * (cosines - margin_value * label_hits.astype(jnp.float32))
    exp_logits = jnp.exp(logits)
    weighted = jnp.dot(
        exp_logits.astype(jnp.bfloat16), centres_unit, preferred_element_type=jnp.float32
    )
    chosen = jnp.dot(
        label_hits.astype(jnp.bfloat16), centres_unit, preferred_element_type=jnp.float32
    )
    totals = jnp.sum(exp_logits, axis=1, keepdims=True)
    sums = jnp.concatenate([weighted, chosen, totals], axis=1).astype(jnp.bfloat16)
    sums = lax.all_to_all(sums.reshape(shards, micro, -1), "shard", 0, 0, tiled=True)
    sums = jnp.sum(sums.astype(jnp.float32), axis=0)
    width = embedded.shape[-1]
    grad_unit = scale_value * (
        sums[:, :width] / sums[:, 2 * width :] - sums[:, width : 2 * width]
    )
    inner = jnp.sum(embedded * grad_unit, axis=-1, keepdims=True)
    grad_embed = factor * (grad_unit - embedded * inner / (width * (squares + tiny_value)))
    grad_pooled = lax.dot_general(
        grad_embed.astype(jnp.bfloat16),
        embed_weight,
        (((1,), (1,)), ((), ())),
        preferred_element_type=jnp.float32,
    )
    g = (grad_pooled[:, None, :] * pool_weight[None]).astype(jnp.bfloat16)

    store = jnp.zeros((2, micro, ROWS, C), jnp.bfloat16)
    for s in reversed(range(planes)):
        g, store = backward_stage(flags[s], g, f1, f2, vec, z, store)
        if s > 0:
            g = lax.ppermute(g, "section", [(2 * s + c, 2 * s - 2 + c) for c in range(2)])

    def narrowed(rows):
        return rows.reshape(-1, SIDE, WIDE, C)[:, :, :SIDE].reshape(-1, SIDE * SIDE, C)

    kept = narrowed(lax.dynamic_index_in_dim(store, core, 0, keepdims=False))
    given = narrowed(lax.dynamic_index_in_dim(store, 1 - core, 0, keepdims=False))
    taken = lax.ppermute(given, "section", swap)
    first = jnp.where(core == 0, kept, taken)
    second = jnp.where(core == 0, taken, kept)
    return jnp.concatenate([first, second], axis=0)[None, :, None]


def solution(mesh):
    placed = (
        P(None, "shard", None, None),
        P("section", None, None),
        P("section", None, None),
        P("section", None),
        P("section", None),
        P("section", None),
        P(),
        P(),
        P("shard", None),
        P(),
        P("shard"),
    )
    return jax.shard_map(
        on_device,
        mesh=mesh,
        in_specs=placed,
        out_specs=P("section", None, "shard", None, None),
        check_vma=False,
    )
```

```python
import functools
import math

import jax
import jax.numpy as jnp
from jax import lax
from jax.experimental import pallas as pl
from jax.experimental.pallas import tpu as pltpu
from jax.sharding import PartitionSpec as P

SIDE = 14
WIDE = 16
ROWS = SIDE * WIDE
C = 256

margin_value = 0.4
scale_value = 64.0
tiny_value = 1e-06

VM = pl.BlockSpec(memory_space=pltpu.VMEM)
HB = pl.BlockSpec(memory_space=pltpu.HBM)
SM = pl.BlockSpec(memory_space=pltpu.SMEM)
LIMIT = 20 * 1024 * 1024


def keep_columns(rows):
    return (lax.broadcasted_iota(jnp.int32, (rows, C), 0) % WIDE) < SIDE


def build(value, cols):
    parts = (pltpu.roll(value, 1, 0), value, pltpu.roll(value, ROWS - 1, 0))
    for place, part in enumerate(parts):
        cols[WIDE : WIDE + ROWS, place * C : (place + 1) * C] = part.astype(jnp.bfloat16)


def conv(cols, weights):
    acc = None
    for step in range(3):
        part = jnp.dot(
            cols[WIDE * step : WIDE * step + ROWS, :],
            weights[step * 3 * C : (step + 1) * 3 * C, :],
            preferred_element_type=jnp.float32,
        )
        acc = part if acc is None else acc + part
    return acc


def clear_border(cols):
    for i in range(cols.shape[0]):
        cols[i, 0:WIDE, :] = jnp.zeros((WIDE, 3 * C), jnp.bfloat16)
        cols[i, WIDE + ROWS :, :] = jnp.zeros((WIDE, 3 * C), jnp.bfloat16)


def start_weights(core, sources, held, sems, order):
    def start(own_unit):
        for u, k in order:
            source = sources[0][k] if u == own_unit else sources[1][k]
            pltpu.make_async_copy(source, held.at[u, k], sems.at[u, k]).start()

    @pl.when(core == 0)
    def _():
        start(0)

    @pl.when(core == 1)
    def _():
        start(1)


def forward_body(
    flag, x_ref, own1, own2, peer1, peer2, vec_ref, out_ref, z_ref, cols, run, zed, held, sems, zsem
):
    @pl.when(flag[0] == 1)
    def _():
        sources = ((own1, own2), (peer1, peer2))
        start_weights(flag[1], sources, held, sems, ((0, 0), (0, 1), (1, 0), (1, 1)))
        clear_border(cols)
        keep = keep_columns(ROWS)
        for i in range(2):
            run[i] = x_ref[i].astype(jnp.float32)

        def one(u, carry):
            vec = vec_ref[u]
            for i in range(2):
                build(run[i], cols.at[2 * i])
            pltpu.make_async_copy(own1, held.at[u, 0], sems.at[u, 0]).wait()
            for i in range(2):
                pre = conv(cols.at[2 * i], held.at[u, 0]) * vec[0:1] + vec[1:2]
                zed[u, i * ROWS : (i + 1) * ROWS] = pre
                leak = vec[2:3]
                four = 4.0 * pre
                soft = jnp.maximum(four, 0.0) + jnp.log1p(jnp.exp(-jnp.abs(four)))
                active = leak * pre + (1.0 - leak) * soft * 0.25
                build(jnp.where(keep, active, 0.0), cols.at[2 * i + 1])
            pltpu.make_async_copy(own2, held.at[u, 1], sems.at[u, 1]).wait()
            for i in range(2):
                result = run[i] + conv(cols.at[2 * i + 1], held.at[u, 1])
                result = jnp.where(keep, result, 0.0).astype(jnp.bfloat16)
                run[i] = result.astype(jnp.float32)
            pltpu.make_async_copy(zed.at[u], z_ref.at[u], zsem.at[u]).start()
            return carry

        lax.fori_loop(0, 2, one, 0)
        for i in range(2):
            out_ref[i] = run[i].astype(jnp.bfloat16)
        for u in range(2):
            pltpu.make_async_copy(zed.at[u], z_ref.at[u], zsem.at[u]).wait()


def backward_body(
    flag, g_ref, own1, own2, peer1, peer2, vec_ref, z_ref, store_in,
    out_ref, store, cols, run, zed, held, sems, zsem,
):
    @pl.when(flag[0] == 1)
    def _():
        sources = ((own1, own2), (peer1, peer2))
        start_weights(flag[1], sources, held, sems, ((1, 1), (1, 0), (0, 1), (0, 0)))
        for u in (1, 0):
            pltpu.make_async_copy(z_ref.at[u], zed.at[u], zsem.at[u]).start()
        clear_border(cols)
        keep = keep_columns(ROWS)
        for i in range(2):
            run[i] = g_ref[i].astype(jnp.float32)

        def one(step, carry):
            u = 1 - step
            vec = vec_ref[u]
            for i in range(2):
                build(run[i], cols.at[2 * i])
            pltpu.make_async_copy(own2, held.at[u, 1], sems.at[u, 1]).wait()
            pltpu.make_async_copy(z_ref.at[u], zed.at[u], zsem.at[u]).wait()
            for i in range(2):
                pre = zed[u, i * ROWS : (i + 1) * ROWS]
                leak = vec[2:3]
                slope = leak + (1.0 - leak) / (1.0 + jnp.exp(-4.0 * pre))
                hidden = conv(cols.at[2 * i], held.at[u, 1]) * slope * vec[0:1]
                build(jnp.where(keep, hidden, 0.0), cols.at[2 * i + 1])
            pltpu.make_async_copy(own1, held.at[u, 0], sems.at[u, 0]).wait()
            for i in range(2):
                result = run[i] + conv(cols.at[2 * i + 1], held.at[u, 0])
                result = jnp.where(keep, result, 0.0).astype(jnp.bfloat16)
                run[i] = result.astype(jnp.float32)
                store[u, i] = result
            return carry

        lax.fori_loop(0, 2, one, 0)
        for i in range(2):
            out_ref[i] = run[i].astype(jnp.bfloat16)


def in_hbm(*arrays):
    return [pltpu.with_memory_space_constraint(a, pltpu.HBM) for a in arrays]


CONV_COST = pl.CostEstimate(flops=4 * 2 * 448 * 2304 * 256, bytes_accessed=6_000_000, transcendentals=500_000)


def stage_scratch(images):
    return [
        pltpu.VMEM((2 * images, ROWS + 2 * WIDE, 3 * C), jnp.bfloat16),
        pltpu.VMEM((images, ROWS, C), jnp.float32),
        pltpu.VMEM((2, images * ROWS, C), jnp.float32),
        pltpu.VMEM((2, 2, 9 * C, C), jnp.bfloat16),
        pltpu.SemaphoreType.DMA((2, 2)),
        pltpu.SemaphoreType.DMA((2,)),
    ]


def forward_stage(flag, x, weights, vec):
    images = x.shape[0]
    return pl.pallas_call(
        forward_body,
        in_specs=[SM, VM, HB, HB, HB, HB, VM],
        out_specs=[VM, HB],
        out_shape=[
            jax.ShapeDtypeStruct(x.shape, jnp.bfloat16),
            pltpu.HBM((2, images * ROWS, C), jnp.float32),
        ],
        scratch_shapes=stage_scratch(images),
        compiler_params=pltpu.CompilerParams(vmem_limit_bytes=LIMIT),
        cost_estimate=CONV_COST,
        name="forward_stage",
    )(flag, x, *in_hbm(*weights), vec)


def backward_stage(flag, g, weights, vec, z, store):
    images = g.shape[0]
    return pl.pallas_call(
        backward_body,
        in_specs=[SM, VM, HB, HB, HB, HB, VM, HB, VM],
        out_specs=[VM, VM],
        out_shape=[
            jax.ShapeDtypeStruct(g.shape, jnp.bfloat16),
            jax.ShapeDtypeStruct(store.shape, store.dtype),
        ],
        scratch_shapes=stage_scratch(images),
        input_output_aliases={8: 1},
        compiler_params=pltpu.CompilerParams(vmem_limit_bytes=LIMIT),
        cost_estimate=CONV_COST,
        name="backward_stage",
    )(flag, g, *in_hbm(*weights), vec, *in_hbm(z), store)


def flip_body(*refs):
    eye = (
        lax.broadcasted_iota(jnp.int32, (C, C), 0) == lax.broadcasted_iota(jnp.int32, (C, C), 1)
    ).astype(jnp.float32).astype(jnp.bfloat16)
    half = len(refs) // 2
    for source, target in zip(refs[:half], refs[half:]):
        turned = lax.dot_general(
            eye, source[...], (((1,), (1,)), ((), ())), preferred_element_type=jnp.float32
        )
        target[...] = turned.astype(jnp.bfloat16)


def flip_all(weights):
    count = len(weights)
    return pl.pallas_call(
        flip_body,
        grid=(9,),
        in_specs=[pl.BlockSpec((C, C), lambda t: (t, 0))] * count,
        out_specs=[pl.BlockSpec((C, C), lambda t: (8 - t, 0))] * count,
        out_shape=[pltpu.HBM(w.shape, w.dtype) for w in weights],
        compiler_params=pltpu.CompilerParams(vmem_limit_bytes=LIMIT),
        cost_estimate=pl.CostEstimate(flops=36 * 2 * 256**3, bytes_accessed=9_000_000, transcendentals=0),
        name="flip_all",
    )(*in_hbm(*weights))


def unit_scale(values):
    squares = jnp.mean(values * values, axis=-1, keepdims=True)
    factor = lax.rsqrt(squares + tiny_value) / math.sqrt(values.shape[-1])
    return (values * factor, squares, factor)


def on_device(
    section_input,
    conv_one,
    conv_two,
    unit_gain,
    offset_bias,
    leak_slope,
    depthwise,
    embed_weight,
    class_centers,
    labels,
    class_offsets,
):
    sections = lax.axis_size("section")
    shards = lax.axis_size("shard")
    planes = sections // 2
    section_index = lax.axis_index("section")
    plane = section_index // 2
    core = section_index % 2
    swap = [(s, s ^ 1) for s in range(sections)]

    def stacked(own):
        peer = lax.ppermute(own, "section", swap)
        both = jnp.zeros((2, *own.shape), own.dtype)
        both = lax.dynamic_update_index_in_dim(both, own, core, 0)
        return lax.dynamic_update_index_in_dim(both, peer, 1 - core, 0)

    own = (conv_one[0], conv_two[0])
    peer = tuple(lax.ppermute(w, "section", swap) for w in own)
    weights = (*own, *peer)
    vec = stacked(jnp.concatenate([unit_gain, offset_bias, leak_slope], axis=0))
    micro = section_input.shape[0] // 2

    def widened(rows):
        grid = rows.reshape(-1, SIDE, SIDE, C)
        return jnp.pad(grid, ((0, 0), (0, 0), (0, WIDE - SIDE), (0, 0))).reshape(-1, ROWS, C)

    mine = lax.dynamic_slice_in_dim(section_input[:, 0], core * micro, micro, 0)
    x = widened(mine)
    pool_weight = widened(depthwise)[0].astype(jnp.float32)
    flags = [jnp.stack([(plane == s).astype(jnp.int32), core]) for s in range(planes)]
    flips = flip_all(weights)
    saved = []
    for s in range(planes):
        x, z = forward_stage(flags[s], x, weights, vec)
        saved.append(z)
        if s < planes - 1:
            x = lax.ppermute(x, "section", [(2 * s + c, 2 * s + 2 + c) for c in range(2)])

    pooled = jnp.sum(x.astype(jnp.float32) * pool_weight[None], axis=1).astype(jnp.bfloat16)
    embedded = jnp.dot(pooled, embed_weight, preferred_element_type=jnp.float32)
    normed, squares, factor = unit_scale(embedded)
    sent = jnp.broadcast_to(normed.astype(jnp.bfloat16)[None], (shards, *normed.shape))
    unit_half = lax.all_to_all(sent, "shard", 0, 0, tiled=True).reshape(shards * micro, -1)
    centres_unit = unit_scale(class_centers.astype(jnp.float32))[0].astype(jnp.bfloat16)
    class_ids = class_offsets[0] + jnp.arange(class_centers.shape[0], dtype=jnp.int32)
    my_labels = lax.dynamic_slice_in_dim(labels, core * micro, micro, 0).T.reshape(-1)
    label_hits = my_labels[:, None] == class_ids[None, :]
    cosines = lax.dot_general(
        unit_half, centres_unit, (((1,), (1,)), ((), ())), preferred_element_type=jnp.float32
    )
    logits = scale_value * (cosines - margin_value * label_hits.astype(jnp.float32))
    exp_logits = jnp.exp(logits)
    weighted = jnp.dot(
        exp_logits.astype(jnp.bfloat16), centres_unit, preferred_element_type=jnp.float32
    )
    chosen = jnp.dot(
        label_hits.astype(jnp.bfloat16), centres_unit, preferred_element_type=jnp.float32
    )
    totals = jnp.sum(exp_logits, axis=1, keepdims=True)
    sums = jnp.concatenate([weighted, chosen, totals], axis=1).astype(jnp.bfloat16)
    sums = lax.all_to_all(sums.reshape(shards, micro, -1), "shard", 0, 0, tiled=True)
    sums = jnp.sum(sums.astype(jnp.float32), axis=0)
    width = embedded.shape[-1]
    grad_unit = scale_value * (
        sums[:, :width] / sums[:, 2 * width :] - sums[:, width : 2 * width]
    )
    inner = jnp.sum(embedded * grad_unit, axis=-1, keepdims=True)
    grad_embed = factor * (grad_unit - embedded * inner / (width * (squares + tiny_value)))
    grad_pooled = lax.dot_general(
        grad_embed.astype(jnp.bfloat16),
        embed_weight,
        (((1,), (1,)), ((), ())),
        preferred_element_type=jnp.float32,
    )
    g = (grad_pooled[:, None, :] * pool_weight[None]).astype(jnp.bfloat16)

    store = jnp.zeros((2, micro, ROWS, C), jnp.bfloat16)
    for s in reversed(range(planes)):
        g, store = backward_stage(flags[s], g, flips, vec, saved[s], store)
        if s > 0:
            g = lax.ppermute(g, "section", [(2 * s + c, 2 * s - 2 + c) for c in range(2)])

    def narrowed(rows):
        return rows.reshape(-1, SIDE, WIDE, C)[:, :, :SIDE].reshape(-1, SIDE * SIDE, C)

    kept = narrowed(lax.dynamic_index_in_dim(store, core, 0, keepdims=False))
    given = narrowed(lax.dynamic_index_in_dim(store, 1 - core, 0, keepdims=False))
    taken = lax.ppermute(given, "section", swap)
    first = jnp.where(core == 0, kept, taken)
    second = jnp.where(core == 0, taken, kept)
    return jnp.concatenate([first, second], axis=0)[None, :, None]


def solution(mesh):
    placed = (
        P(None, "shard", None, None),
        P("section", None, None),
        P("section", None, None),
        P("section", None),
        P("section", None),
        P("section", None),
        P(),
        P(),
        P("shard", None),
        P(),
        P("shard"),
    )
    return jax.shard_map(
        on_device,
        mesh=mesh,
        in_specs=placed,
        out_specs=P("section", None, "shard", None, None),
        check_vma=False,
    )
```

```python
import functools
import math

import jax
import jax.numpy as jnp
from jax import lax
from jax.experimental import pallas as pl
from jax.experimental.pallas import tpu as pltpu
from jax.sharding import PartitionSpec as P

SIDE = 14
WIDE = 16
ROWS = SIDE * WIDE
C = 256

margin_value = 0.4
scale_value = 64.0
tiny_value = 1e-06

VM = pl.BlockSpec(memory_space=pltpu.VMEM)
HB = pl.BlockSpec(memory_space=pltpu.HBM)
SM = pl.BlockSpec(memory_space=pltpu.SMEM)
LIMIT = 20 * 1024 * 1024


def keep_columns(rows):
    return (lax.broadcasted_iota(jnp.int32, (rows, C), 0) % WIDE) < SIDE


HALF = ROWS // 2


def build(value, cols, base):
    rows = value.shape[0]
    parts = (pltpu.roll(value, 1, 0), value, pltpu.roll(value, rows - 1, 0))
    for place, part in enumerate(parts):
        cols[WIDE + base : WIDE + base + rows, place * C : (place + 1) * C] = part.astype(jnp.bfloat16)


def conv(cols, weights, base):
    acc = None
    for step in range(3):
        part = jnp.dot(
            cols[base + WIDE * step : base + WIDE * step + HALF, :],
            weights[step * 3 * C : (step + 1) * 3 * C, :],
            preferred_element_type=jnp.float32,
        )
        acc = part if acc is None else acc + part
    return acc


def clear_border(cols):
    for i in range(2):
        cols[i, 0:WIDE, :] = jnp.zeros((WIDE, 3 * C), jnp.bfloat16)
        cols[i, WIDE + ROWS :, :] = jnp.zeros((WIDE, 3 * C), jnp.bfloat16)


HALVES = tuple(slice(h * HALF, (h + 1) * HALF) for h in range(2))


def load_body(flag, own1, own2, peer1, peer2, *rest):
    held, sems = rest[-2:]
    for k, source in enumerate((own1, own2)):
        pltpu.make_async_copy(source, held.at[flag[0], k], sems.at[0, k]).start()
    for k, source in enumerate((peer1, peer2)):
        pltpu.make_async_copy(source, held.at[1 - flag[0], k], sems.at[1, k]).start()
    for k, source in enumerate((own1, own2)):
        pltpu.make_async_copy(source, held.at[flag[0], k], sems.at[0, k]).wait()
    for k, source in enumerate((peer1, peer2)):
        pltpu.make_async_copy(source, held.at[1 - flag[0], k], sems.at[1, k]).wait()


def forward_body(flag, x_ref, held, vec_ref, out_ref, z_ref, cols, run, zed, zsem):
    @pl.when(flag[0] == 1)
    def _():
        clear_border(cols)
        keep = keep_columns(HALF)
        run[...] = x_ref[0].astype(jnp.float32)

        def one(u, carry):
            vec = vec_ref[u]
            for h in HALVES:
                build(run[h], cols.at[0], h.start)
            for h in HALVES:
                pre = conv(cols.at[0], held.at[u, 0], h.start) * vec[0:1] + vec[1:2]
                zed[u, h] = pre.astype(jnp.bfloat16)
                leak = vec[2:3]
                rest = jnp.log(1.0 + jnp.exp(-4.0 * jnp.abs(pre)))
                active = pre * jnp.where(pre < 0.0, leak, 1.0) + (0.25 * (1.0 - leak)) * rest
                build(jnp.where(keep, active, 0.0), cols.at[1], h.start)
            pltpu.make_async_copy(zed.at[u], z_ref.at[u], zsem.at[u]).start()
            for h in HALVES:
                result = run[h] + conv(cols.at[1], held.at[u, 1], h.start)
                result = jnp.where(keep, result, 0.0).astype(jnp.bfloat16)
                run[h] = result.astype(jnp.float32)
            return carry

        lax.fori_loop(0, 2, one, 0)
        out_ref[0] = run[...].astype(jnp.bfloat16)
        for u in range(2):
            pltpu.make_async_copy(zed.at[u], z_ref.at[u], zsem.at[u]).wait()


def backward_body(flag, g_ref, held, vec_ref, z_ref, store_in, out_ref, store, cols, run, zed, zsem):
    @pl.when(flag[0] == 1)
    def _():
        for u in (1, 0):
            pltpu.make_async_copy(z_ref.at[u], zed.at[u], zsem.at[u]).start()
        clear_border(cols)
        keep = keep_columns(HALF)
        run[...] = g_ref[0].astype(jnp.float32)

        def one(step, carry):
            u = 1 - step
            vec = vec_ref[u]
            for h in HALVES:
                build(run[h], cols.at[0], h.start)
            pltpu.make_async_copy(z_ref.at[u], zed.at[u], zsem.at[u]).wait()
            for h in HALVES:
                pre = zed[u, h].astype(jnp.float32)
                half = 0.5 * vec[0:1]
                slope = half * (1.0 + vec[2:3]) + half * (1.0 - vec[2:3]) * jnp.tanh(2.0 * pre)
                hidden = conv(cols.at[0], held.at[u, 1], h.start) * slope
                build(jnp.where(keep, hidden, 0.0), cols.at[1], h.start)
            for h in HALVES:
                result = run[h] + conv(cols.at[1], held.at[u, 0], h.start)
                result = jnp.where(keep, result, 0.0).astype(jnp.bfloat16)
                run[h] = result.astype(jnp.float32)
                store[u, h] = result
            return carry

        lax.fori_loop(0, 2, one, 0)
        out_ref[0] = run[...].astype(jnp.bfloat16)


def in_hbm(*arrays):
    return [pltpu.with_memory_space_constraint(a, pltpu.HBM) for a in arrays]


CONV_COST = pl.CostEstimate(flops=4 * 2 * 224 * 2304 * 256, bytes_accessed=6_000_000, transcendentals=250_000)
STAGE_LIMIT = 8 * 1024 * 1024
STAGE_SCRATCH = [
    pltpu.VMEM((2, ROWS + 2 * WIDE, 3 * C), jnp.bfloat16),
    pltpu.VMEM((ROWS, C), jnp.float32),
    pltpu.VMEM((2, ROWS, C), jnp.bfloat16),
    pltpu.SemaphoreType.DMA((2,)),
]


def load_weights(core, weights, name, before=()):
    return pl.pallas_call(
        load_body,
        in_specs=[SM, HB, HB, HB, HB] + [pl.BlockSpec(memory_space=pl.ANY)] * len(before),
        out_specs=VM,
        out_shape=jax.ShapeDtypeStruct((2, 2, *weights[0].shape), weights[0].dtype),
        scratch_shapes=[pltpu.SemaphoreType.DMA((2, 2))],
        compiler_params=pltpu.CompilerParams(vmem_limit_bytes=STAGE_LIMIT),
        cost_estimate=pl.CostEstimate(flops=300_000_000, bytes_accessed=9_000_000, transcendentals=0),
        name=name,
    )(core, *in_hbm(*weights), *before)


def forward_stage(flag, x, held, vec):
    return pl.pallas_call(
        forward_body,
        in_specs=[SM, VM, VM, VM],
        out_specs=[VM, HB],
        out_shape=[
            jax.ShapeDtypeStruct(x.shape, jnp.bfloat16),
            pltpu.HBM((2, ROWS, C), jnp.bfloat16),
        ],
        scratch_shapes=STAGE_SCRATCH,
        compiler_params=pltpu.CompilerParams(vmem_limit_bytes=STAGE_LIMIT),
        cost_estimate=CONV_COST,
        name="forward_stage",
    )(flag, x, held, vec)


def backward_stage(flag, g, held, vec, z, store):
    return pl.pallas_call(
        backward_body,
        in_specs=[SM, VM, VM, VM, HB, VM],
        out_specs=[VM, VM],
        out_shape=[
            jax.ShapeDtypeStruct(g.shape, jnp.bfloat16),
            jax.ShapeDtypeStruct(store.shape, store.dtype),
        ],
        scratch_shapes=STAGE_SCRATCH,
        input_output_aliases={5: 1},
        compiler_params=pltpu.CompilerParams(vmem_limit_bytes=STAGE_LIMIT),
        cost_estimate=CONV_COST,
        name="backward_stage",
    )(flag, g, held, vec, *in_hbm(z), store)


def flip_body(*refs):
    eye = (
        lax.broadcasted_iota(jnp.int32, (C, C), 0) == lax.broadcasted_iota(jnp.int32, (C, C), 1)
    ).astype(jnp.float32).astype(jnp.bfloat16)
    half = len(refs) // 2
    for source, target in zip(refs[:half], refs[half:]):
        turned = lax.dot_general(
            eye, source[...], (((1,), (1,)), ((), ())), preferred_element_type=jnp.float32
        )
        target[...] = turned.astype(jnp.bfloat16)


def flip_all(weights):
    count = len(weights)
    return pl.pallas_call(
        flip_body,
        grid=(9,),
        in_specs=[pl.BlockSpec((C, C), lambda t: (t, 0))] * count,
        out_specs=[pl.BlockSpec((C, C), lambda t: (8 - t, 0))] * count,
        out_shape=[pltpu.HBM(w.shape, w.dtype) for w in weights],
        compiler_params=pltpu.CompilerParams(vmem_limit_bytes=LIMIT),
        cost_estimate=pl.CostEstimate(flops=36 * 2 * 256**3, bytes_accessed=9_000_000, transcendentals=0),
        name="flip_all",
    )(*in_hbm(*weights))


def unit_scale(values):
    squares = jnp.mean(values * values, axis=-1, keepdims=True)
    factor = lax.rsqrt(squares + tiny_value) / math.sqrt(values.shape[-1])
    return (values * factor, squares, factor)


def on_device(
    section_input,
    conv_one,
    conv_two,
    unit_gain,
    offset_bias,
    leak_slope,
    depthwise,
    embed_weight,
    class_centers,
    labels,
    class_offsets,
):
    sections = lax.axis_size("section")
    shards = lax.axis_size("shard")
    planes = sections // 2
    section_index = lax.axis_index("section")
    plane = section_index // 2
    core = section_index % 2
    swap = [(s, s ^ 1) for s in range(sections)]

    def stacked(own):
        peer = lax.ppermute(own, "section", swap)
        both = jnp.zeros((2, *own.shape), own.dtype)
        both = lax.dynamic_update_index_in_dim(both, own, core, 0)
        return lax.dynamic_update_index_in_dim(both, peer, 1 - core, 0)

    own = (conv_one[0], conv_two[0])
    peer = tuple(lax.ppermute(w, "section", swap) for w in own)
    weights = (*own, *peer)
    vec = stacked(jnp.concatenate([unit_gain, offset_bias, leak_slope], axis=0))
    micro = section_input.shape[0] // 2

    def widened(rows):
        grid = rows.reshape(-1, SIDE, SIDE, C)
        return jnp.pad(grid, ((0, 0), (0, 0), (0, WIDE - SIDE), (0, 0))).reshape(-1, ROWS, C)

    mine = lax.dynamic_slice_in_dim(section_input[:, 0], core * micro, micro, 0)
    x = widened(mine)
    flags = [(plane == s).astype(jnp.int32).reshape(1) for s in range(planes)]
    flips = flip_all(weights)
    parts = [x[m : m + 1] for m in range(micro)]
    class_ids = class_offsets[0] + jnp.arange(class_centers.shape[0], dtype=jnp.int32)
    held = load_weights(core.reshape(1), weights, "load_forward", (*parts, class_ids, *flags))
    saved = {}
    for s in range(planes):
        for m in range(micro):
            parts[m], saved[s, m] = forward_stage(flags[s], parts[m], held, vec)
            if s < planes - 1:
                parts[m] = lax.ppermute(parts[m], "section", [(2 * s + c, 2 * s + 2 + c) for c in range(2)])
    x = jnp.concatenate(parts, axis=0)
    x, depthwise, embed_weight, class_centers, labels = lax.optimization_barrier(
        (x, depthwise, embed_weight, class_centers, labels)
    )
    pool_weight = widened(depthwise)[0].astype(jnp.float32)
    pooled = jnp.sum(x.astype(jnp.float32) * pool_weight[None], axis=1).astype(jnp.bfloat16)
    embedded = jnp.dot(pooled, embed_weight, preferred_element_type=jnp.float32)
    normed, squares, factor = unit_scale(embedded)
    sent = jnp.broadcast_to(normed.astype(jnp.bfloat16)[None], (shards, *normed.shape))
    unit_half = lax.all_to_all(sent, "shard", 0, 0, tiled=True).reshape(shards * micro, -1)
    centres_unit = unit_scale(class_centers.astype(jnp.float32))[0].astype(jnp.bfloat16)
    my_labels = lax.dynamic_slice_in_dim(labels, core * micro, micro, 0).T.reshape(-1)
    label_hits = my_labels[:, None] == class_ids[None, :]
    cosines = lax.dot_general(
        unit_half, centres_unit, (((1,), (1,)), ((), ())), preferred_element_type=jnp.float32
    )
    logits = scale_value * (cosines - margin_value * label_hits.astype(jnp.float32))
    exp_logits = jnp.exp(logits)
    weighted = jnp.dot(
        exp_logits.astype(jnp.bfloat16), centres_unit, preferred_element_type=jnp.float32
    )
    chosen = jnp.dot(
        label_hits.astype(jnp.bfloat16), centres_unit, preferred_element_type=jnp.float32
    )
    totals = jnp.sum(exp_logits, axis=1, keepdims=True)
    sums = jnp.concatenate([weighted, chosen, totals], axis=1).astype(jnp.bfloat16)
    sums = lax.all_to_all(sums.reshape(shards, micro, -1), "shard", 0, 0, tiled=True)
    sums = jnp.sum(sums.astype(jnp.float32), axis=0)
    width = embedded.shape[-1]
    grad_unit = scale_value * (
        sums[:, :width] / sums[:, 2 * width :] - sums[:, width : 2 * width]
    )
    inner = jnp.sum(embedded * grad_unit, axis=-1, keepdims=True)
    grad_embed = factor * (grad_unit - embedded * inner / (width * (squares + tiny_value)))
    grad_pooled = lax.dot_general(
        grad_embed.astype(jnp.bfloat16),
        embed_weight,
        (((1,), (1,)), ((), ())),
        preferred_element_type=jnp.float32,
    )
    g = (grad_pooled[:, None, :] * pool_weight[None]).astype(jnp.bfloat16)

    flips, g = lax.optimization_barrier((flips, g))
    flips = load_weights(core.reshape(1), flips, "load_backward")
    parts = [g[m : m + 1] for m in range(micro)]
    stores = [jnp.zeros((2, ROWS, C), jnp.bfloat16) for m in range(micro)]
    for s in reversed(range(planes)):
        for m in range(micro):
            parts[m], stores[m] = backward_stage(flags[s], parts[m], flips, vec, saved[s, m], stores[m])
            if s > 0:
                parts[m] = lax.ppermute(parts[m], "section", [(2 * s + c, 2 * s - 2 + c) for c in range(2)])
    store = jnp.stack(stores, axis=1)

    def narrowed(rows):
        return rows.reshape(-1, SIDE, WIDE, C)[:, :, :SIDE].reshape(-1, SIDE * SIDE, C)

    kept = narrowed(lax.dynamic_index_in_dim(store, core, 0, keepdims=False))
    given = narrowed(lax.dynamic_index_in_dim(store, 1 - core, 0, keepdims=False))
    taken = lax.ppermute(given, "section", swap)
    first = jnp.where(core == 0, kept, taken)
    second = jnp.where(core == 0, taken, kept)
    return jnp.concatenate([first, second], axis=0)[None, :, None]


def solution(mesh):
    placed = (
        P(None, "shard", None, None),
        P("section", None, None),
        P("section", None, None),
        P("section", None),
        P("section", None),
        P("section", None),
        P(),
        P(),
        P("shard", None),
        P(),
        P("shard"),
    )
    return jax.shard_map(
        on_device,
        mesh=mesh,
        in_specs=placed,
        out_specs=P("section", None, "shard", None, None),
        check_vma=False,
    )
```

```python
import functools
import math

import jax
import jax.numpy as jnp
from jax import lax
from jax.experimental import pallas as pl
from jax.experimental.pallas import tpu as pltpu
from jax.sharding import PartitionSpec as P

SIDE = 14
WIDE = 16
ROWS = SIDE * WIDE
C = 256

margin_value = 0.4
scale_value = 64.0
tiny_value = 1e-06

VM = pl.BlockSpec(memory_space=pltpu.VMEM)
AN = pl.BlockSpec(memory_space=pl.ANY)
HB = pl.BlockSpec(memory_space=pltpu.HBM)
SM = pl.BlockSpec(memory_space=pltpu.SMEM)
LIMIT = 20 * 1024 * 1024


def keep_columns(rows):
    return (lax.broadcasted_iota(jnp.int32, (rows, C), 0) % WIDE) < SIDE


HALF = ROWS // 2


def build(value, cols, base):
    rows = value.shape[0]
    parts = (pltpu.roll(value, 1, 0), value, pltpu.roll(value, rows - 1, 0))
    for place, part in enumerate(parts):
        cols[WIDE + base : WIDE + base + rows, place * C : (place + 1) * C] = part.astype(jnp.bfloat16)


def conv(cols, weights, base):
    acc = None
    for step in range(3):
        part = jnp.dot(
            cols[base + WIDE * step : base + WIDE * step + HALF, :],
            weights[step * 3 * C : (step + 1) * 3 * C, :],
            preferred_element_type=jnp.float32,
        )
        acc = part if acc is None else acc + part
    return acc


def clear_border(cols):
    for i in range(2):
        cols[i, 0:WIDE, :] = jnp.zeros((WIDE, 3 * C), jnp.bfloat16)
        cols[i, WIDE + ROWS :, :] = jnp.zeros((WIDE, 3 * C), jnp.bfloat16)


HALVES = tuple(slice(h * HALF, (h + 1) * HALF) for h in range(2))


def load_body(flag, own1, own2, peer1, peer2, *rest):
    held, sems = rest[-2:]
    for k, source in enumerate((own1, own2)):
        pltpu.make_async_copy(source, held.at[flag[0], k], sems.at[0, k]).start()
    for k, source in enumerate((peer1, peer2)):
        pltpu.make_async_copy(source, held.at[1 - flag[0], k], sems.at[1, k]).start()
    for k, source in enumerate((own1, own2)):
        pltpu.make_async_copy(source, held.at[flag[0], k], sems.at[0, k]).wait()
    for k, source in enumerate((peer1, peer2)):
        pltpu.make_async_copy(source, held.at[1 - flag[0], k], sems.at[1, k]).wait()


def forward_body(flag, x_ref, held, vec_ref, out_ref, z_ref, cols, run, zed, zsem):
    @pl.when(flag[0] == 1)
    def _():
        clear_border(cols)
        keep = keep_columns(HALF)
        run[...] = x_ref[0].astype(jnp.float32)

        def one(u, carry):
            vec = vec_ref[u]
            for h in HALVES:
                build(run[h], cols.at[0], h.start)
            for h in HALVES:
                pre = conv(cols.at[0], held.at[u, 0], h.start) * vec[0:1] + vec[1:2]
                zed[u, h] = pre.astype(jnp.bfloat16)
                leak = vec[2:3]
                rest = jnp.log(1.0 + jnp.exp(-4.0 * jnp.abs(pre)))
                active = pre * jnp.where(pre < 0.0, leak, 1.0) + (0.25 * (1.0 - leak)) * rest
                build(jnp.where(keep, active, 0.0), cols.at[1], h.start)
            pltpu.make_async_copy(zed.at[u], z_ref.at[u], zsem.at[u]).start()
            for h in HALVES:
                result = run[h] + conv(cols.at[1], held.at[u, 1], h.start)
                result = jnp.where(keep, result, 0.0).astype(jnp.bfloat16)
                run[h] = result.astype(jnp.float32)
            return carry

        lax.fori_loop(0, 2, one, 0)
        out_ref[0] = run[...].astype(jnp.bfloat16)
        for u in range(2):
            pltpu.make_async_copy(zed.at[u], z_ref.at[u], zsem.at[u]).wait()


def backward_body(image, flag, g_ref, held, vec_ref, z_ref, store_in, out_ref, store, cols, run):
    @pl.when(flag[0] == 1)
    def _():
        clear_border(cols)
        keep = keep_columns(HALF)
        run[...] = g_ref[0].astype(jnp.float32)

        def one(step, carry):
            u = 1 - step
            vec = vec_ref[u]
            half = 0.5 * vec[0:1]
            base = half * (1.0 + vec[2:3])
            gain = half * (1.0 - vec[2:3])
            for h in HALVES:
                build(run[h], cols.at[0], h.start)
            for h in HALVES:
                slope = base + gain * jnp.tanh(2.0 * z_ref[image, u, h].astype(jnp.float32))
                hidden = conv(cols.at[0], held.at[u, 1], h.start) * slope
                build(jnp.where(keep, hidden, 0.0), cols.at[1], h.start)
            for h in HALVES:
                result = run[h] + conv(cols.at[1], held.at[u, 0], h.start)
                result = jnp.where(keep, result, 0.0).astype(jnp.bfloat16)
                run[h] = result.astype(jnp.float32)
                store[u, h] = result
            return carry

        lax.fori_loop(0, 2, one, 0)
        out_ref[0] = run[...].astype(jnp.bfloat16)


def tail_body(
    flag, sums_ref, chosen_ref, embedded_ref, embed_ref, pool_ref, own1, own2, peer1, peer2, *rest
):
    saved, (g_ref, held, zbuf, sems, zsems) = rest[:-5], rest[-5:]
    images = zbuf.shape[0]
    core, plane = flag[0], flag[1]
    copies = [
        pltpu.make_async_copy(source, held.at[place, k], sems.at[side, k])
        for side, place, pair in ((0, core, (own1, own2)), (1, 1 - core, (peer1, peer2)))
        for k, source in enumerate(pair)
    ]
    for copy in copies:
        copy.start()
    for s in range(len(saved) // images):

        @pl.when(plane == s)
        def _():
            for m in range(images):
                pltpu.make_async_copy(saved[s * images + m], zbuf.at[m], zsems.at[m]).start()

    embedded = embedded_ref[...]
    width = embedded.shape[1]
    squares = jnp.sum(embedded * embedded, axis=1, keepdims=True) / width
    factor = lax.rsqrt(squares + tiny_value) / math.sqrt(width)
    total = sums_ref[:, width : width + 1]
    grad_unit = scale_value * (sums_ref[:, :width] / total - chosen_ref[...].astype(jnp.float32))
    inner = jnp.sum(embedded * grad_unit, axis=1, keepdims=True)
    grad_embed = factor * (grad_unit - embedded * inner / (width * (squares + tiny_value)))
    grad_pooled = lax.dot_general(
        grad_embed.astype(jnp.bfloat16),
        embed_ref[...],
        (((1,), (1,)), ((), ())),
        preferred_element_type=jnp.float32,
    )
    for m in range(images):
        g_ref[m] = (grad_pooled[m : m + 1] * pool_ref[...]).astype(jnp.bfloat16)
    for copy in copies:
        copy.wait()
    for m in range(images):
        pltpu.make_async_copy(saved[m], zbuf.at[m], zsems.at[m]).wait()


def tail(flag, sums, chosen, embedded, embed_weight, pool_weight, weights, saved):
    images = sums.shape[0]
    return pl.pallas_call(
        tail_body,
        in_specs=[SM, VM, VM, VM, VM, VM] + [HB] * (len(weights) + len(saved)),
        out_specs=[VM, VM, VM],
        out_shape=[
            jax.ShapeDtypeStruct((images, ROWS, C), jnp.bfloat16),
            jax.ShapeDtypeStruct((2, 2, *weights[0].shape), weights[0].dtype),
            jax.ShapeDtypeStruct((images, 2, ROWS, C), jnp.bfloat16),
        ],
        scratch_shapes=[pltpu.SemaphoreType.DMA((2, 2)), pltpu.SemaphoreType.DMA((images,))],
        compiler_params=pltpu.CompilerParams(vmem_limit_bytes=STAGE_LIMIT),
        cost_estimate=pl.CostEstimate(flops=300_000_000, bytes_accessed=9_000_000, transcendentals=0),
        name="tail",
    )(flag, sums, chosen, embedded, embed_weight, pool_weight, *in_hbm(*weights), *in_hbm(*saved))


def in_hbm(*arrays):
    return [pltpu.with_memory_space_constraint(a, pltpu.HBM) for a in arrays]


CONV_COST = pl.CostEstimate(flops=4 * 2 * 224 * 2304 * 256, bytes_accessed=6_000_000, transcendentals=250_000)
STAGE_LIMIT = 8 * 1024 * 1024
STAGE_SCRATCH = [
    pltpu.VMEM((2, ROWS + 2 * WIDE, 3 * C), jnp.bfloat16),
    pltpu.VMEM((ROWS, C), jnp.float32),
    pltpu.VMEM((2, ROWS, C), jnp.bfloat16),
    pltpu.SemaphoreType.DMA((2,)),
]


def load_weights(core, weights, name, before=()):
    return pl.pallas_call(
        load_body,
        in_specs=[SM, HB, HB, AN, AN] + [AN] * len(before),
        out_specs=VM,
        out_shape=jax.ShapeDtypeStruct((2, 2, *weights[0].shape), weights[0].dtype),
        scratch_shapes=[pltpu.SemaphoreType.DMA((2, 2))],
        compiler_params=pltpu.CompilerParams(vmem_limit_bytes=STAGE_LIMIT),
        cost_estimate=pl.CostEstimate(flops=300_000_000, bytes_accessed=9_000_000, transcendentals=0),
        name=name,
    )(core, *in_hbm(*weights[:2]), *weights[2:], *before)


def forward_stage(flag, x, held, vec):
    return pl.pallas_call(
        forward_body,
        in_specs=[SM, VM, VM, VM],
        out_specs=[VM, HB],
        out_shape=[
            jax.ShapeDtypeStruct(x.shape, jnp.bfloat16),
            pltpu.HBM((2, ROWS, C), jnp.bfloat16),
        ],
        scratch_shapes=STAGE_SCRATCH,
        compiler_params=pltpu.CompilerParams(vmem_limit_bytes=STAGE_LIMIT),
        cost_estimate=CONV_COST,
        name="forward_stage",
    )(flag, x, held, vec)


def backward_stage(image, flag, g, held, vec, z, store):
    return pl.pallas_call(
        functools.partial(backward_body, image),
        in_specs=[SM, VM, VM, VM, VM, VM],
        out_specs=[VM, VM],
        out_shape=[
            jax.ShapeDtypeStruct(g.shape, jnp.bfloat16),
            jax.ShapeDtypeStruct(store.shape, store.dtype),
        ],
        scratch_shapes=STAGE_SCRATCH[:2],
        input_output_aliases={5: 1},
        compiler_params=pltpu.CompilerParams(vmem_limit_bytes=STAGE_LIMIT),
        cost_estimate=CONV_COST,
        name="backward_stage",
    )(flag, g, held, vec, z, store)


def flip_body(*refs):
    eye = (
        lax.broadcasted_iota(jnp.int32, (C, C), 0) == lax.broadcasted_iota(jnp.int32, (C, C), 1)
    ).astype(jnp.float32).astype(jnp.bfloat16)
    half = len(refs) // 2
    for source, target in zip(refs[:half], refs[half:]):
        turned = lax.dot_general(
            eye, source[...], (((1,), (1,)), ((), ())), preferred_element_type=jnp.float32
        )
        target[...] = turned.astype(jnp.bfloat16)


def flip_all(weights):
    count = len(weights)
    return pl.pallas_call(
        flip_body,
        grid=(9,),
        in_specs=[pl.BlockSpec((C, C), lambda t: (t, 0))] * count,
        out_specs=[pl.BlockSpec((C, C), lambda t: (8 - t, 0))] * count,
        out_shape=[pltpu.HBM(w.shape, w.dtype) for w in weights],
        compiler_params=pltpu.CompilerParams(vmem_limit_bytes=LIMIT),
        cost_estimate=pl.CostEstimate(flops=36 * 2 * 256**3, bytes_accessed=9_000_000, transcendentals=0),
        name="flip_all",
    )(*in_hbm(*weights))


def unit_scale(values):
    squares = jnp.mean(values * values, axis=-1, keepdims=True)
    factor = lax.rsqrt(squares + tiny_value) / math.sqrt(values.shape[-1])
    return (values * factor, squares, factor)


def on_device(
    section_input,
    conv_one,
    conv_two,
    unit_gain,
    offset_bias,
    leak_slope,
    depthwise,
    embed_weight,
    class_centers,
    labels,
    class_offsets,
):
    sections = lax.axis_size("section")
    shards = lax.axis_size("shard")
    planes = sections // 2
    section_index = lax.axis_index("section")
    plane = section_index // 2
    core = section_index % 2
    swap = [(s, s ^ 1) for s in range(sections)]

    def stacked(own):
        peer = lax.ppermute(own, "section", swap)
        both = jnp.zeros((2, *own.shape), own.dtype)
        both = lax.dynamic_update_index_in_dim(both, own, core, 0)
        return lax.dynamic_update_index_in_dim(both, peer, 1 - core, 0)

    own = (conv_one[0], conv_two[0])
    peer = tuple(lax.ppermute(w, "section", swap) for w in own)
    weights = (*own, *peer)
    vec = stacked(jnp.concatenate([unit_gain, offset_bias, leak_slope], axis=0))
    micro = section_input.shape[0] // 2

    def widened(rows):
        grid = rows.reshape(-1, SIDE, SIDE, C)
        return jnp.pad(grid, ((0, 0), (0, 0), (0, WIDE - SIDE), (0, 0))).reshape(-1, ROWS, C)

    mine = lax.dynamic_slice_in_dim(section_input[:, 0], core * micro, micro, 0)
    x = widened(mine)
    flags = [(plane == s).astype(jnp.int32).reshape(1) for s in range(planes)]
    flips = flip_all(weights)
    parts = [x[m : m + 1] for m in range(micro)]
    class_ids = class_offsets[0] + jnp.arange(class_centers.shape[0], dtype=jnp.int32)
    held = load_weights(core.reshape(1), weights, "load_forward", (*parts, class_ids, *flags))
    saved = {}
    for s in range(planes):
        for m in range(micro):
            parts[m], saved[s, m] = forward_stage(flags[s], parts[m], held, vec)
            if s < planes - 1:
                parts[m] = lax.ppermute(parts[m], "section", [(2 * s + c, 2 * s + 2 + c) for c in range(2)])
    x = jnp.concatenate(parts, axis=0)
    x, depthwise, embed_weight, class_centers, labels = lax.optimization_barrier(
        (x, depthwise, embed_weight, class_centers, labels)
    )
    pool_weight = widened(depthwise)[0].astype(jnp.float32)
    pooled = jnp.sum(x.astype(jnp.float32) * pool_weight[None], axis=1).astype(jnp.bfloat16)
    embedded = jnp.dot(pooled, embed_weight, preferred_element_type=jnp.float32)
    normed = unit_scale(embedded)[0]
    width = embedded.shape[-1]
    my_labels = lax.dynamic_slice_in_dim(labels, core * micro, micro, 0).T.reshape(-1)

    def scaled_centres():
        return unit_scale(class_centers.astype(jnp.float32))[0].astype(jnp.bfloat16)

    def label_rows():
        hits = my_labels[:, None] == class_ids[None, :]
        rows = jnp.dot(
            hits.astype(jnp.bfloat16), scaled_centres(), preferred_element_type=jnp.float32
        ).astype(jnp.bfloat16)
        rows = lax.all_to_all(rows.reshape(shards, micro, width), "shard", 0, 0, tiled=True)
        return jnp.sum(rows.astype(jnp.float32), axis=0).astype(jnp.bfloat16)

    chosen = lax.cond(plane == 0, label_rows, lambda: jnp.zeros((micro, width), jnp.bfloat16))
    chosen = lax.ppermute(chosen, "section", [(c, sections - 2 + c) for c in range(2)])
    sent = jnp.broadcast_to(normed.astype(jnp.bfloat16)[None], (shards, micro, width))
    unit_half = lax.all_to_all(sent, "shard", 0, 0, tiled=True).reshape(shards * micro, width)
    centres_unit = scaled_centres()
    label_hits = my_labels[:, None] == class_ids[None, :]
    cosines = lax.dot_general(
        unit_half, centres_unit, (((1,), (1,)), ((), ())), preferred_element_type=jnp.float32
    )
    logits = scale_value * (cosines - margin_value * label_hits.astype(jnp.float32))
    exp_logits = jnp.exp(logits)
    weighted = jnp.dot(
        exp_logits.astype(jnp.bfloat16), centres_unit, preferred_element_type=jnp.float32
    )
    totals = jnp.sum(exp_logits, axis=1, keepdims=True)
    sums = jnp.concatenate([weighted, totals], axis=1).astype(jnp.bfloat16)
    sums = lax.all_to_all(sums.reshape(shards, micro, -1), "shard", 0, 0, tiled=True)
    sums = jnp.sum(sums.astype(jnp.float32), axis=0)
    g, flips, zbuf = tail(
        jnp.stack([core, plane]), sums, chosen, embedded, embed_weight, pool_weight, flips,
        [saved[s, m] for s in range(planes) for m in range(micro)],
    )
    parts = [g[m : m + 1] for m in range(micro)]
    stores = [jnp.zeros((2, ROWS, C), jnp.bfloat16) for m in range(micro)]
    for s in reversed(range(planes)):
        for m in range(micro):
            parts[m], stores[m] = backward_stage(m, flags[s], parts[m], flips, vec, zbuf, stores[m])
            if s > 0:
                parts[m] = lax.ppermute(parts[m], "section", [(2 * s + c, 2 * s - 2 + c) for c in range(2)])
    store = jnp.stack(stores, axis=1)

    def narrowed(rows):
        return rows.reshape(-1, SIDE, WIDE, C)[:, :, :SIDE].reshape(-1, SIDE * SIDE, C)

    kept = narrowed(lax.dynamic_index_in_dim(store, core, 0, keepdims=False))
    given = narrowed(lax.dynamic_index_in_dim(store, 1 - core, 0, keepdims=False))
    taken = lax.ppermute(given, "section", swap)
    first = jnp.where(core == 0, kept, taken)
    second = jnp.where(core == 0, taken, kept)
    return jnp.concatenate([first, second], axis=0)[None, :, None]


def solution(mesh):
    placed = (
        P(None, "shard", None, None),
        P("section", None, None),
        P("section", None, None),
        P("section", None),
        P("section", None),
        P("section", None),
        P(),
        P(),
        P("shard", None),
        P(),
        P("shard"),
    )
    return jax.shard_map(
        on_device,
        mesh=mesh,
        in_specs=placed,
        out_specs=P("section", None, "shard", None, None),
        check_vma=False,
    )
```

```python
import functools
import math

import jax
import jax.numpy as jnp
from jax import lax
from jax.experimental import pallas as pl
from jax.experimental.pallas import tpu as pltpu
from jax.sharding import PartitionSpec as P

SIDE = 14
WIDE = 16
ROWS = SIDE * WIDE
C = 256

margin_value = 0.4
scale_value = 64.0
tiny_value = 1e-06

VM = pl.BlockSpec(memory_space=pltpu.VMEM)
AN = pl.BlockSpec(memory_space=pl.ANY)
HB = pl.BlockSpec(memory_space=pltpu.HBM)
SM = pl.BlockSpec(memory_space=pltpu.SMEM)
LIMIT = 20 * 1024 * 1024


def keep_columns(rows):
    return (lax.broadcasted_iota(jnp.int32, (rows, C), 0) % WIDE) < SIDE


HALF = ROWS // 2


def build(value, cols, base):
    rows = value.shape[0]
    parts = (pltpu.roll(value, 1, 0), value, pltpu.roll(value, rows - 1, 0))
    for place, part in enumerate(parts):
        cols[WIDE + base : WIDE + base + rows, place * C : (place + 1) * C] = part.astype(jnp.bfloat16)


def conv(cols, weights, base):
    acc = None
    for step in range(3):
        part = jnp.dot(
            cols[base + WIDE * step : base + WIDE * step + HALF, :],
            weights[step * 3 * C : (step + 1) * 3 * C, :],
            preferred_element_type=jnp.float32,
        )
        acc = part if acc is None else acc + part
    return acc


def clear_border(cols):
    for i in range(2):
        cols[i, 0:WIDE, :] = jnp.zeros((WIDE, 3 * C), jnp.bfloat16)
        cols[i, WIDE + ROWS :, :] = jnp.zeros((WIDE, 3 * C), jnp.bfloat16)


HALVES = tuple(slice(h * HALF, (h + 1) * HALF) for h in range(2))


def load_body(flag, own1, own2, peer1, peer2, own_vec, peer_vec, pool, embed, *rest):
    held, vec, pool_out, embed_out, sems, more = rest[-6:]
    core = flag[0]
    copies = [
        pltpu.make_async_copy(source, held.at[place, k], sems.at[side, k])
        for side, place, pair in ((0, core, (own1, own2)), (1, 1 - core, (peer1, peer2)))
        for k, source in enumerate(pair)
    ] + [
        pltpu.make_async_copy(pool, pool_out, more.at[0]),
        pltpu.make_async_copy(embed, embed_out, more.at[1]),
    ]
    for copy in copies:
        copy.start()
    vec[core] = own_vec[...]
    vec[1 - core] = peer_vec[...]
    for copy in copies:
        copy.wait()


def pool_body(first, second, pool_ref, embed_ref, embedded_ref, sent_ref):
    pooled = []
    for image in (first, second):
        total = jnp.zeros((SIDE, C), jnp.float32)
        for i in range(SIDE):
            rows = image[0, WIDE * i : WIDE * i + SIDE, :].astype(jnp.float32)
            total += rows * pool_ref[SIDE * i : SIDE * i + SIDE, :].astype(jnp.float32)
        pooled.append(jnp.sum(total, axis=0, keepdims=True))
    pooled = jnp.concatenate(pooled, axis=0).astype(jnp.bfloat16)
    embedded = jnp.dot(pooled, embed_ref[...], preferred_element_type=jnp.float32)
    embedded_ref[...] = embedded
    normed = unit_scale(embedded)[0].astype(jnp.bfloat16)
    sent_ref[...] = jnp.broadcast_to(normed[None], sent_ref.shape)


def pool_and_embed(parts, pool, embed, shards):
    width = embed.shape[1]
    return pl.pallas_call(
        pool_body,
        in_specs=[VM] * 4,
        out_specs=[VM, VM],
        out_shape=[
            jax.ShapeDtypeStruct((2, width), jnp.float32),
            jax.ShapeDtypeStruct((shards, 2, width), jnp.bfloat16),
        ],
        compiler_params=pltpu.CompilerParams(vmem_limit_bytes=STAGE_LIMIT),
        cost_estimate=pl.CostEstimate(flops=100_000_000, bytes_accessed=1_000_000, transcendentals=0),
        name="pool_and_embed",
    )(*parts, pool, embed)


def centres_body(centres_ref, after, out_ref):
    values = centres_ref[...].astype(jnp.float32)
    out_ref[...] = unit_scale(values)[0].astype(jnp.bfloat16)


def unit_centres(centres, after):
    rows, width = centres.shape
    block = pl.BlockSpec((128, width), lambda i: (i, 0))
    return pl.pallas_call(
        centres_body,
        grid=(rows // 128,),
        in_specs=[block, AN],
        out_specs=block,
        out_shape=jax.ShapeDtypeStruct(centres.shape, jnp.bfloat16),
        compiler_params=pltpu.CompilerParams(vmem_limit_bytes=STAGE_LIMIT),
        cost_estimate=pl.CostEstimate(flops=100_000_000, bytes_accessed=3_000_000, transcendentals=0),
        name="unit_centres",
    )(*in_hbm(centres), after)


def forward_body(flag, x_ref, held, vec_ref, out_ref, z_ref, cols, run, zed, zsem):
    @pl.when(flag[0] == 1)
    def _():
        clear_border(cols)
        keep = keep_columns(HALF)
        run[...] = x_ref[0].astype(jnp.float32)

        def one(u, carry):
            vec = vec_ref[u]
            for h in HALVES:
                build(run[h], cols.at[0], h.start)
            for h in HALVES:
                pre = conv(cols.at[0], held.at[u, 0], h.start) * vec[0:1] + vec[1:2]
                zed[u, h] = pre.astype(jnp.bfloat16)
                leak = vec[2:3]
                rest = jnp.log(1.0 + jnp.exp(-4.0 * jnp.abs(pre)))
                active = pre * jnp.where(pre < 0.0, leak, 1.0) + (0.25 * (1.0 - leak)) * rest
                build(jnp.where(keep, active, 0.0), cols.at[1], h.start)
            pltpu.make_async_copy(zed.at[u], z_ref.at[u], zsem.at[u]).start()
            for h in HALVES:
                result = run[h] + conv(cols.at[1], held.at[u, 1], h.start)
                result = jnp.where(keep, result, 0.0).astype(jnp.bfloat16)
                run[h] = result.astype(jnp.float32)
            return carry

        lax.fori_loop(0, 2, one, 0)
        out_ref[0] = run[...].astype(jnp.bfloat16)
        for u in range(2):
            pltpu.make_async_copy(zed.at[u], z_ref.at[u], zsem.at[u]).wait()


def backward_body(image, flag, g_ref, held, vec_ref, z_ref, store_in, *rest):
    store, cols, run = rest[-3:]

    @pl.when(flag[0] == 1)
    def _():
        clear_border(cols)
        keep = keep_columns(HALF)
        run[...] = g_ref[0].astype(jnp.float32)

        def one(step, carry):
            u = 1 - step
            vec = vec_ref[u]
            half = 0.5 * vec[0:1]
            base = half * (1.0 + vec[2:3])
            gain = half * (1.0 - vec[2:3])
            for h in HALVES:
                build(run[h], cols.at[0], h.start)
            for h in HALVES:
                slope = base + gain * jnp.tanh(2.0 * z_ref[image, u, h].astype(jnp.float32))
                hidden = conv(cols.at[0], held.at[u, 1], h.start) * slope
                build(jnp.where(keep, hidden, 0.0), cols.at[1], h.start)
            for h in HALVES:
                result = run[h] + conv(cols.at[1], held.at[u, 0], h.start)
                result = jnp.where(keep, result, 0.0).astype(jnp.bfloat16)
                run[h] = result.astype(jnp.float32)
                store[u, h] = result
            return carry

        lax.fori_loop(0, 2, one, 0)
        if rest[0].ndim == 3:
            rest[0][0] = run[...].astype(jnp.bfloat16)


def tail_body(
    flag, sums_ref, chosen_ref, embedded_ref, embed_ref, pool_ref, own1, own2, peer1, peer2, *rest
):
    saved, (g_ref, held, zbuf, sems, zsems) = rest[:-5], rest[-5:]
    images = zbuf.shape[0]
    core, plane = flag[0], flag[1]
    copies = [
        pltpu.make_async_copy(source, held.at[place, k], sems.at[side, k])
        for side, place, pair in ((0, core, (own1, own2)), (1, 1 - core, (peer1, peer2)))
        for k, source in enumerate(pair)
    ]
    for copy in copies:
        copy.start()
    for s in range(len(saved) // images):

        @pl.when(plane == s)
        def _():
            for m in range(images):
                pltpu.make_async_copy(saved[s * images + m], zbuf.at[m], zsems.at[m]).start()

    embedded = embedded_ref[...]
    width = embedded.shape[1]
    squares = jnp.sum(embedded * embedded, axis=1, keepdims=True) / width
    factor = lax.rsqrt(squares + tiny_value) / math.sqrt(width)
    total = sums_ref[:, width : width + 1]
    grad_unit = scale_value * (sums_ref[:, :width] / total - chosen_ref[...].astype(jnp.float32))
    inner = jnp.sum(embedded * grad_unit, axis=1, keepdims=True)
    grad_embed = factor * (grad_unit - embedded * inner / (width * (squares + tiny_value)))
    grad_pooled = lax.dot_general(
        grad_embed.astype(jnp.bfloat16),
        embed_ref[...],
        (((1,), (1,)), ((), ())),
        preferred_element_type=jnp.float32,
    )
    for m in range(images):
        g_ref[m] = (grad_pooled[m : m + 1] * pool_ref[...]).astype(jnp.bfloat16)
    for copy in copies:
        copy.wait()
    for m in range(images):
        pltpu.make_async_copy(saved[m], zbuf.at[m], zsems.at[m]).wait()


def tail(flag, sums, chosen, embedded, embed_weight, pool_weight, weights, saved):
    images = sums.shape[0]
    return pl.pallas_call(
        tail_body,
        in_specs=[SM, VM, VM, VM, VM, VM] + [HB] * (len(weights) + len(saved)),
        out_specs=[VM, VM, VM],
        out_shape=[
            jax.ShapeDtypeStruct((images, ROWS, C), jnp.bfloat16),
            jax.ShapeDtypeStruct((2, 2, *weights[0].shape), weights[0].dtype),
            jax.ShapeDtypeStruct((images, 2, ROWS, C), jnp.bfloat16),
        ],
        scratch_shapes=[pltpu.SemaphoreType.DMA((2, 2)), pltpu.SemaphoreType.DMA((images,))],
        compiler_params=pltpu.CompilerParams(vmem_limit_bytes=STAGE_LIMIT),
        cost_estimate=pl.CostEstimate(flops=300_000_000, bytes_accessed=9_000_000, transcendentals=0),
        name="tail",
    )(flag, sums, chosen, embedded, embed_weight, pool_weight, *in_hbm(*weights), *in_hbm(*saved))


def in_hbm(*arrays):
    return [pltpu.with_memory_space_constraint(a, pltpu.HBM) for a in arrays]


CONV_COST = pl.CostEstimate(flops=4 * 2 * 224 * 2304 * 256, bytes_accessed=6_000_000, transcendentals=250_000)
STAGE_LIMIT = 8 * 1024 * 1024
STAGE_SCRATCH = [
    pltpu.VMEM((2, ROWS + 2 * WIDE, 3 * C), jnp.bfloat16),
    pltpu.VMEM((ROWS, C), jnp.float32),
    pltpu.VMEM((2, ROWS, C), jnp.bfloat16),
    pltpu.SemaphoreType.DMA((2,)),
]


def load_weights(core, weights, own_vec, peer_vec, pool, embed, before):
    return pl.pallas_call(
        load_body,
        in_specs=[SM, HB, HB, AN, AN, VM, VM, HB, HB] + [AN] * len(before),
        out_specs=[VM] * 4,
        out_shape=[
            jax.ShapeDtypeStruct((2, 2, *weights[0].shape), weights[0].dtype),
            jax.ShapeDtypeStruct((2, *own_vec.shape), own_vec.dtype),
            jax.ShapeDtypeStruct(pool.shape, pool.dtype),
            jax.ShapeDtypeStruct(embed.shape, embed.dtype),
        ],
        scratch_shapes=[pltpu.SemaphoreType.DMA((2, 2)), pltpu.SemaphoreType.DMA((2,))],
        compiler_params=pltpu.CompilerParams(vmem_limit_bytes=STAGE_LIMIT),
        cost_estimate=pl.CostEstimate(flops=300_000_000, bytes_accessed=9_000_000, transcendentals=0),
        name="load_weights",
    )(core, *in_hbm(*weights[:2]), *weights[2:], own_vec, peer_vec, *in_hbm(pool, embed), *before)


def forward_stage(flag, x, held, vec):
    return pl.pallas_call(
        forward_body,
        in_specs=[SM, VM, VM, VM],
        out_specs=[VM, HB],
        out_shape=[
            jax.ShapeDtypeStruct(x.shape, jnp.bfloat16),
            pltpu.HBM((2, ROWS, C), jnp.bfloat16),
        ],
        scratch_shapes=STAGE_SCRATCH,
        compiler_params=pltpu.CompilerParams(vmem_limit_bytes=STAGE_LIMIT),
        cost_estimate=CONV_COST,
        name="forward_stage",
    )(flag, x, held, vec)


def backward_stage(image, last, flag, g, held, vec, z, store):
    passed = [jax.ShapeDtypeStruct((16, 128) if last else g.shape, jnp.bfloat16)]
    outs = pl.pallas_call(
        functools.partial(backward_body, image),
        in_specs=[SM, VM, VM, VM, VM, VM],
        out_specs=[VM] * (len(passed) + 1),
        out_shape=passed + [jax.ShapeDtypeStruct(store.shape, store.dtype)],
        scratch_shapes=STAGE_SCRATCH[:2],
        input_output_aliases={5: len(passed)},
        compiler_params=pltpu.CompilerParams(vmem_limit_bytes=STAGE_LIMIT),
        cost_estimate=CONV_COST,
        name="backward_stage",
    )(flag, g, held, vec, z, store)
    return outs[0], outs[-1]


def flip_body(*refs):
    eye = (
        lax.broadcasted_iota(jnp.int32, (C, C), 0) == lax.broadcasted_iota(jnp.int32, (C, C), 1)
    ).astype(jnp.float32).astype(jnp.bfloat16)
    half = len(refs) // 2
    for source, target in zip(refs[:half], refs[half:]):
        turned = lax.dot_general(
            eye, source[...], (((1,), (1,)), ((), ())), preferred_element_type=jnp.float32
        )
        target[...] = turned.astype(jnp.bfloat16)


def flip_all(weights):
    count = len(weights)
    return pl.pallas_call(
        flip_body,
        grid=(9,),
        in_specs=[pl.BlockSpec((C, C), lambda t: (t, 0))] * count,
        out_specs=[pl.BlockSpec((C, C), lambda t: (8 - t, 0))] * count,
        out_shape=[pltpu.HBM(w.shape, w.dtype) for w in weights],
        compiler_params=pltpu.CompilerParams(vmem_limit_bytes=LIMIT),
        cost_estimate=pl.CostEstimate(flops=36 * 2 * 256**3, bytes_accessed=9_000_000, transcendentals=0),
        name="flip_all",
    )(*in_hbm(*weights))


def unit_scale(values):
    squares = jnp.mean(values * values, axis=-1, keepdims=True)
    factor = lax.rsqrt(squares + tiny_value) / math.sqrt(values.shape[-1])
    return (values * factor, squares, factor)


def on_device(
    section_input,
    conv_one,
    conv_two,
    unit_gain,
    offset_bias,
    leak_slope,
    depthwise,
    embed_weight,
    class_centers,
    labels,
    class_offsets,
):
    sections = lax.axis_size("section")
    shards = lax.axis_size("shard")
    planes = sections // 2
    section_index = lax.axis_index("section")
    plane = section_index // 2
    core = section_index % 2
    swap = [(s, s ^ 1) for s in range(sections)]

    own = (conv_one[0], conv_two[0])
    peer = tuple(lax.ppermute(w, "section", swap) for w in own)
    weights = (*own, *peer)
    own_vec = jnp.concatenate([unit_gain, offset_bias, leak_slope], axis=0)
    peer_vec = lax.ppermute(own_vec, "section", swap)
    micro = section_input.shape[0] // 2

    def widened(rows):
        grid = rows.reshape(-1, SIDE, SIDE, C)
        return jnp.pad(grid, ((0, 0), (0, 0), (0, WIDE - SIDE), (0, 0))).reshape(-1, ROWS, C)

    mine = lax.dynamic_slice_in_dim(section_input[:, 0], core * micro, micro, 0)
    x = widened(mine)
    flags = [(plane == s).astype(jnp.int32).reshape(1) for s in range(planes)]
    flips = flip_all(weights)
    parts = [x[m : m + 1] for m in range(micro)]
    mine_at, other_at = core.astype(jnp.uint32), (1 - core).astype(jnp.uint32)
    class_ids = class_offsets[0] + jnp.arange(class_centers.shape[0], dtype=jnp.int32)
    held, vec, pool_compact, embed_ready = load_weights(
        core.reshape(1), weights, own_vec, peer_vec, depthwise, embed_weight, (*parts, class_ids, *flags, mine_at.reshape(1), other_at.reshape(1))
    )
    saved = {}
    for s in range(planes):
        for m in range(micro):
            parts[m], saved[s, m] = forward_stage(flags[s], parts[m], held, vec)
            if s < planes - 1:
                parts[m] = lax.ppermute(parts[m], "section", [(2 * s + c, 2 * s + 2 + c) for c in range(2)])
    embedded, sent = pool_and_embed(parts, pool_compact, embed_ready, shards)
    width = embedded.shape[-1]
    embedded, depthwise, embed_weight, labels = lax.optimization_barrier(
        (embedded, depthwise, embed_weight, labels)
    )
    pool_weight = widened(depthwise)[0].astype(jnp.float32)

    def find_hits():
        mine = lax.dynamic_slice_in_dim(labels, core * micro, micro, 0).T.reshape(-1)
        return mine[:, None] == class_ids[None, :]

    def label_rows():
        rows = jnp.dot(
            find_hits().astype(jnp.bfloat16),
            unit_centres(class_centers, class_ids),
            preferred_element_type=jnp.float32,
        ).astype(jnp.bfloat16)
        rows = lax.all_to_all(rows.reshape(shards, micro, width), "shard", 0, 0, tiled=True)
        return jnp.sum(rows.astype(jnp.float32), axis=0).astype(jnp.bfloat16)

    chosen = lax.cond(plane == 0, label_rows, lambda: jnp.zeros((micro, width), jnp.bfloat16))
    chosen = lax.ppermute(chosen, "section", [(c, sections - 2 + c) for c in range(2)])
    unit_half = lax.all_to_all(sent, "shard", 0, 0, tiled=True).reshape(shards * micro, width)
    centres_unit = unit_centres(class_centers, chosen)
    label_hits = find_hits()
    cosines = lax.dot_general(
        unit_half, centres_unit, (((1,), (1,)), ((), ())), preferred_element_type=jnp.float32
    )
    logits = scale_value * (cosines - margin_value * label_hits.astype(jnp.float32))
    exp_logits = jnp.exp(logits)
    weighted = jnp.dot(
        exp_logits.astype(jnp.bfloat16), centres_unit, preferred_element_type=jnp.float32
    )
    totals = jnp.sum(exp_logits, axis=1, keepdims=True)
    sums = jnp.concatenate([weighted, totals], axis=1).astype(jnp.bfloat16)
    sums = lax.all_to_all(sums.reshape(shards, micro, -1), "shard", 0, 0, tiled=True)
    sums = jnp.sum(sums.astype(jnp.float32), axis=0)
    g, flips, zbuf = tail(
        jnp.stack([core, plane]), sums, chosen, embedded, embed_weight, pool_weight, flips,
        [saved[s, m] for s in range(planes) for m in range(micro)],
    )
    parts = [g[m : m + 1] for m in range(micro)]
    stores = [jnp.zeros((2, ROWS, C), jnp.bfloat16) for m in range(micro)]
    for s in reversed(range(planes)):
        for m in range(micro):
            parts[m], stores[m] = backward_stage(m, s == 0, flags[s], parts[m], flips, vec, zbuf, stores[m])
            if s > 0:
                parts[m] = lax.ppermute(parts[m], "section", [(2 * s + c, 2 * s - 2 + c) for c in range(2)])
    store = jnp.stack(stores, axis=1)

    def narrowed(rows):
        return rows.reshape(-1, SIDE, WIDE, C)[:, :, :SIDE].reshape(-1, SIDE * SIDE, C)

    kept = narrowed(lax.dynamic_index_in_dim(store, mine_at, 0, keepdims=False))
    given = narrowed(lax.dynamic_index_in_dim(store, other_at, 0, keepdims=False))
    taken = lax.ppermute(given, "section", swap)
    first = jnp.where(mine_at == 0, kept, taken)
    second = jnp.where(mine_at == 0, taken, kept)
    return jnp.concatenate([first, second], axis=0)[None, :, None]


def solution(mesh):
    placed = (
        P(None, "shard", None, None),
        P("section", None, None),
        P("section", None, None),
        P("section", None),
        P("section", None),
        P("section", None),
        P(),
        P(),
        P("shard", None),
        P(),
        P("shard"),
    )
    return jax.shard_map(
        on_device,
        mesh=mesh,
        in_specs=placed,
        out_specs=P("section", None, "shard", None, None),
        check_vma=False,
    )
```

```python
import functools
import math

import jax
import jax.numpy as jnp
from jax import lax
from jax.experimental import pallas as pl
from jax.experimental.pallas import tpu as pltpu
from jax.sharding import PartitionSpec as P

SIDE = 14
WIDE = 16
ROWS = SIDE * WIDE
C = 256

margin_value = 0.4
scale_value = 64.0
tiny_value = 1e-06

VM = pl.BlockSpec(memory_space=pltpu.VMEM)
AN = pl.BlockSpec(memory_space=pl.ANY)
HB = pl.BlockSpec(memory_space=pltpu.HBM)
SM = pl.BlockSpec(memory_space=pltpu.SMEM)
LIMIT = 20 * 1024 * 1024


def keep_columns(rows):
    return (lax.broadcasted_iota(jnp.int32, (rows, C), 0) % WIDE) < SIDE


HALF = ROWS // 2


def build(value, cols, base):
    rows = value.shape[0]
    parts = (pltpu.roll(value, 1, 0), value, pltpu.roll(value, rows - 1, 0))
    for place, part in enumerate(parts):
        cols[WIDE + base : WIDE + base + rows, place * C : (place + 1) * C] = part.astype(jnp.bfloat16)


def conv(cols, weights, base):
    acc = None
    for step in range(3):
        part = jnp.dot(
            cols[base + WIDE * step : base + WIDE * step + HALF, :],
            weights[step * 3 * C : (step + 1) * 3 * C, :],
            preferred_element_type=jnp.float32,
        )
        acc = part if acc is None else acc + part
    return acc


def clear_border(cols):
    for i in range(2):
        cols[i, 0:WIDE, :] = jnp.zeros((WIDE, 3 * C), jnp.bfloat16)
        cols[i, WIDE + ROWS :, :] = jnp.zeros((WIDE, 3 * C), jnp.bfloat16)


HALVES = tuple(slice(h * HALF, (h + 1) * HALF) for h in range(2))


def load_body(flag, own1, own2, peer1, peer2, own_vec, peer_vec, pool, embed, *rest):
    held, vec, pool_out, embed_out, sems, more = rest[-6:]
    core = flag[0]
    copies = [
        pltpu.make_async_copy(source, held.at[place, k], sems.at[side, k])
        for side, place, pair in ((0, core, (own1, own2)), (1, 1 - core, (peer1, peer2)))
        for k, source in enumerate(pair)
    ] + [
        pltpu.make_async_copy(pool, pool_out, more.at[0]),
        pltpu.make_async_copy(embed, embed_out, more.at[1]),
    ]
    for copy in copies:
        copy.start()
    vec[core] = own_vec[...]
    vec[1 - core] = peer_vec[...]
    for copy in copies:
        copy.wait()


def pool_body(first, second, pool_ref, embed_ref, embedded_ref, sent_ref):
    pooled = []
    for image in (first, second):
        total = jnp.zeros((SIDE, C), jnp.float32)
        for i in range(SIDE):
            rows = image[0, WIDE * i : WIDE * i + SIDE, :].astype(jnp.float32)
            total += rows * pool_ref[SIDE * i : SIDE * i + SIDE, :].astype(jnp.float32)
        pooled.append(jnp.sum(total, axis=0, keepdims=True))
    pooled = jnp.concatenate(pooled, axis=0).astype(jnp.bfloat16)
    embedded = jnp.dot(pooled, embed_ref[...], preferred_element_type=jnp.float32)
    embedded_ref[...] = embedded
    normed = unit_scale(embedded)[0].astype(jnp.bfloat16)
    sent_ref[...] = jnp.broadcast_to(normed[None], sent_ref.shape)


def pool_and_embed(parts, pool, embed, shards):
    width = embed.shape[1]
    return pl.pallas_call(
        pool_body,
        in_specs=[VM] * 4,
        out_specs=[VM, VM],
        out_shape=[
            jax.ShapeDtypeStruct((2, width), jnp.float32),
            jax.ShapeDtypeStruct((shards, 2, width), jnp.bfloat16),
        ],
        compiler_params=pltpu.CompilerParams(vmem_limit_bytes=STAGE_LIMIT),
        cost_estimate=pl.CostEstimate(flops=100_000_000, bytes_accessed=1_000_000, transcendentals=0),
        name="pool_and_embed",
    )(*parts, pool, embed)


def head_body(unit_ref, centres_ref, scale_ref, labels_ref, ids_ref, *rest):
    out_ref = rest[-1]
    faces = unit_ref.shape[0]
    width = centres_ref.shape[1]
    centres = centres_ref[...]
    scale = scale_ref[...]
    cosines = lax.dot_general(
        unit_ref[...], centres, (((1,), (1,)), ((), ())), preferred_element_type=jnp.float32
    )
    hits = (labels_ref[...] == ids_ref[...]).astype(jnp.float32)
    weights = jnp.exp(scale_value * (cosines * scale - margin_value * hits))
    totals = jnp.sum(weights, axis=1, keepdims=True)
    weighted = jnp.dot(
        (weights * scale).astype(jnp.bfloat16), centres, preferred_element_type=jnp.float32
    )
    out_ref[:, :width] = weighted.astype(jnp.bfloat16)
    out_ref[:, width:] = jnp.broadcast_to(totals, (faces, 128)).astype(jnp.bfloat16)


def class_sums(unit_half, centres, scale, labels, ids, after):
    faces, width = unit_half.shape
    return pl.pallas_call(
        head_body,
        in_specs=[VM] * 5 + [AN] * len(after),
        out_specs=VM,
        out_shape=jax.ShapeDtypeStruct((faces, width + 128), jnp.bfloat16),
        compiler_params=pltpu.CompilerParams(vmem_limit_bytes=STAGE_LIMIT),
        cost_estimate=pl.CostEstimate(flops=450_000_000, bytes_accessed=2_000_000, transcendentals=220_000),
        name="class_sums",
    )(unit_half, centres, scale, labels, ids, *in_hbm(*after))


def forward_body(flag, x_ref, held, vec_ref, out_ref, z_ref, cols, run, zed, zsem):
    @pl.when(flag[0] == 1)
    def _():
        clear_border(cols)
        keep = keep_columns(HALF)
        run[...] = x_ref[0].astype(jnp.float32)

        def one(u, carry):
            vec = vec_ref[u]
            for h in HALVES:
                build(run[h], cols.at[0], h.start)
            for h in HALVES:
                pre = conv(cols.at[0], held.at[u, 0], h.start) * vec[0:1] + vec[1:2]
                zed[u, h] = pre.astype(jnp.bfloat16)
                leak = vec[2:3]
                rest = jnp.log(1.0 + jnp.exp(-4.0 * jnp.abs(pre)))
                active = pre * jnp.where(pre < 0.0, leak, 1.0) + (0.25 * (1.0 - leak)) * rest
                build(jnp.where(keep, active, 0.0), cols.at[1], h.start)
            pltpu.make_async_copy(zed.at[u], z_ref.at[u], zsem.at[u]).start()
            for h in HALVES:
                result = run[h] + conv(cols.at[1], held.at[u, 1], h.start)
                result = jnp.where(keep, result, 0.0).astype(jnp.bfloat16)
                run[h] = result.astype(jnp.float32)
            return carry

        lax.fori_loop(0, 2, one, 0)
        out_ref[0] = run[...].astype(jnp.bfloat16)
        for u in range(2):
            pltpu.make_async_copy(zed.at[u], z_ref.at[u], zsem.at[u]).wait()


def backward_body(image, flag, g_ref, held, vec_ref, z_ref, store_in, *rest):
    store, cols, run = rest[-3:]

    @pl.when(flag[0] == 1)
    def _():
        clear_border(cols)
        keep = keep_columns(HALF)
        run[...] = g_ref[0].astype(jnp.float32)

        def one(step, carry):
            u = 1 - step
            vec = vec_ref[u]
            half = 0.5 * vec[0:1]
            base = half * (1.0 + vec[2:3])
            gain = half * (1.0 - vec[2:3])
            for h in HALVES:
                build(run[h], cols.at[0], h.start)
            for h in HALVES:
                slope = base + gain * jnp.tanh(2.0 * z_ref[image, u, h].astype(jnp.float32))
                hidden = conv(cols.at[0], held.at[u, 1], h.start) * slope
                build(jnp.where(keep, hidden, 0.0), cols.at[1], h.start)
            for h in HALVES:
                result = run[h] + conv(cols.at[1], held.at[u, 0], h.start)
                result = jnp.where(keep, result, 0.0).astype(jnp.bfloat16)
                run[h] = result.astype(jnp.float32)
                store[u, h] = result
            return carry

        lax.fori_loop(0, 2, one, 0)
        if len(rest) == 4:
            rest[0][0] = run[...].astype(jnp.bfloat16)


def tail_body(
    flag, sums_ref, chosen_ref, embedded_ref, embed_ref, pool_ref, own1, own2, peer1, peer2, *rest
):
    saved, (g_ref, held, zbuf, sems, zsems) = rest[:-5], rest[-5:]
    images = zbuf.shape[0]
    core, plane = flag[0], flag[1]
    copies = [
        pltpu.make_async_copy(source, held.at[place, k], sems.at[side, k])
        for side, place, pair in ((0, core, (own1, own2)), (1, 1 - core, (peer1, peer2)))
        for k, source in enumerate(pair)
    ]
    for copy in copies:
        copy.start()
    for s in range(len(saved) // images):

        @pl.when(plane == s)
        def _():
            for m in range(images):
                pltpu.make_async_copy(saved[s * images + m], zbuf.at[m], zsems.at[m]).start()

    embedded = embedded_ref[...]
    width = embedded.shape[1]
    squares = jnp.sum(embedded * embedded, axis=1, keepdims=True) / width
    factor = lax.rsqrt(squares + tiny_value) / math.sqrt(width)
    total = sums_ref[:, width : width + 1]
    grad_unit = scale_value * (sums_ref[:, :width] / total - chosen_ref[...].astype(jnp.float32))
    inner = jnp.sum(embedded * grad_unit, axis=1, keepdims=True)
    grad_embed = factor * (grad_unit - embedded * inner / (width * (squares + tiny_value)))
    grad_pooled = lax.dot_general(
        grad_embed.astype(jnp.bfloat16),
        embed_ref[...],
        (((1,), (1,)), ((), ())),
        preferred_element_type=jnp.float32,
    )
    for m in range(images):
        g_ref[m] = (grad_pooled[m : m + 1] * pool_ref[...]).astype(jnp.bfloat16)
    for copy in copies:
        copy.wait()
    for m in range(images):
        pltpu.make_async_copy(saved[m], zbuf.at[m], zsems.at[m]).wait()


def tail(flag, sums, chosen, embedded, embed_weight, pool_weight, weights, saved):
    images = sums.shape[0]
    return pl.pallas_call(
        tail_body,
        in_specs=[SM, VM, VM, VM, VM, VM] + [HB] * (len(weights) + len(saved)),
        out_specs=[VM, VM, VM],
        out_shape=[
            jax.ShapeDtypeStruct((images, ROWS, C), jnp.bfloat16),
            jax.ShapeDtypeStruct((2, 2, *weights[0].shape), weights[0].dtype),
            jax.ShapeDtypeStruct((images, 2, ROWS, C), jnp.bfloat16),
        ],
        scratch_shapes=[pltpu.SemaphoreType.DMA((2, 2)), pltpu.SemaphoreType.DMA((images,))],
        compiler_params=pltpu.CompilerParams(vmem_limit_bytes=STAGE_LIMIT),
        cost_estimate=pl.CostEstimate(flops=300_000_000, bytes_accessed=9_000_000, transcendentals=0),
        name="tail",
    )(flag, sums, chosen, embedded, embed_weight, pool_weight, *in_hbm(*weights), *in_hbm(*saved))


def in_hbm(*arrays):
    return [pltpu.with_memory_space_constraint(a, pltpu.HBM) for a in arrays]


CONV_COST = pl.CostEstimate(flops=4 * 2 * 224 * 2304 * 256, bytes_accessed=6_000_000, transcendentals=250_000)
STAGE_LIMIT = 8 * 1024 * 1024
STAGE_SCRATCH = [
    pltpu.VMEM((2, ROWS + 2 * WIDE, 3 * C), jnp.bfloat16),
    pltpu.VMEM((ROWS, C), jnp.float32),
    pltpu.VMEM((2, ROWS, C), jnp.bfloat16),
    pltpu.SemaphoreType.DMA((2,)),
]


def load_weights(core, weights, own_vec, peer_vec, pool, embed, before):
    return pl.pallas_call(
        load_body,
        in_specs=[SM, HB, HB, AN, AN, VM, VM, HB, HB] + [AN] * len(before),
        out_specs=[VM] * 4,
        out_shape=[
            jax.ShapeDtypeStruct((2, 2, *weights[0].shape), weights[0].dtype),
            jax.ShapeDtypeStruct((2, *own_vec.shape), own_vec.dtype),
            jax.ShapeDtypeStruct(pool.shape, pool.dtype),
            jax.ShapeDtypeStruct(embed.shape, embed.dtype),
        ],
        scratch_shapes=[pltpu.SemaphoreType.DMA((2, 2)), pltpu.SemaphoreType.DMA((2,))],
        compiler_params=pltpu.CompilerParams(vmem_limit_bytes=STAGE_LIMIT),
        cost_estimate=pl.CostEstimate(flops=300_000_000, bytes_accessed=9_000_000, transcendentals=0),
        name="load_weights",
    )(core, *in_hbm(*weights[:2]), *weights[2:], own_vec, peer_vec, *in_hbm(pool, embed), *before)


def forward_stage(flag, x, held, vec):
    return pl.pallas_call(
        forward_body,
        in_specs=[SM, VM, VM, VM],
        out_specs=[VM, HB],
        out_shape=[
            jax.ShapeDtypeStruct(x.shape, jnp.bfloat16),
            pltpu.HBM((2, ROWS, C), jnp.bfloat16),
        ],
        scratch_shapes=STAGE_SCRATCH,
        compiler_params=pltpu.CompilerParams(vmem_limit_bytes=STAGE_LIMIT),
        cost_estimate=CONV_COST,
        name="forward_stage",
    )(flag, x, held, vec)


def backward_stage(image, last, flag, g, held, vec, z, store):
    passed = [] if last else [jax.ShapeDtypeStruct(g.shape, jnp.bfloat16)]
    outs = pl.pallas_call(
        functools.partial(backward_body, image),
        in_specs=[SM, VM, VM, VM, VM, VM],
        out_specs=[VM] * (len(passed) + 1),
        out_shape=passed + [jax.ShapeDtypeStruct(store.shape, store.dtype)],
        scratch_shapes=STAGE_SCRATCH[:2],
        input_output_aliases={5: len(passed)},
        compiler_params=pltpu.CompilerParams(vmem_limit_bytes=STAGE_LIMIT),
        cost_estimate=CONV_COST,
        name="backward_stage",
    )(flag, g, held, vec, z, store)
    return outs[0], outs[-1]


def flip_body(*refs):
    eye = (
        lax.broadcasted_iota(jnp.int32, (C, C), 0) == lax.broadcasted_iota(jnp.int32, (C, C), 1)
    ).astype(jnp.float32).astype(jnp.bfloat16)
    half = len(refs) // 2
    for source, target in zip(refs[:half], refs[half:]):
        turned = lax.dot_general(
            eye, source[...], (((1,), (1,)), ((), ())), preferred_element_type=jnp.float32
        )
        target[...] = turned.astype(jnp.bfloat16)


def flip_all(weights):
    count = len(weights)
    return pl.pallas_call(
        flip_body,
        grid=(9,),
        in_specs=[pl.BlockSpec((C, C), lambda t: (t, 0))] * count,
        out_specs=[pl.BlockSpec((C, C), lambda t: (8 - t, 0))] * count,
        out_shape=[pltpu.HBM(w.shape, w.dtype) for w in weights],
        compiler_params=pltpu.CompilerParams(vmem_limit_bytes=LIMIT),
        cost_estimate=pl.CostEstimate(flops=36 * 2 * 256**3, bytes_accessed=9_000_000, transcendentals=0),
        name="flip_all",
    )(*in_hbm(*weights))


def unit_scale(values):
    squares = jnp.mean(values * values, axis=-1, keepdims=True)
    factor = lax.rsqrt(squares + tiny_value) / math.sqrt(values.shape[-1])
    return (values * factor, squares, factor)


def on_device(
    section_input,
    conv_one,
    conv_two,
    unit_gain,
    offset_bias,
    leak_slope,
    depthwise,
    embed_weight,
    class_centers,
    labels,
    class_offsets,
):
    sections = lax.axis_size("section")
    shards = lax.axis_size("shard")
    planes = sections // 2
    section_index = lax.axis_index("section")
    plane = section_index // 2
    core = section_index % 2
    swap = [(s, s ^ 1) for s in range(sections)]

    own = (conv_one[0], conv_two[0])
    peer = tuple(lax.ppermute(w, "section", swap) for w in own)
    weights = (*own, *peer)
    own_vec = jnp.concatenate([unit_gain, offset_bias, leak_slope], axis=0)
    peer_vec = lax.ppermute(own_vec, "section", swap)
    micro = section_input.shape[0] // 2

    def widened(rows):
        grid = rows.reshape(-1, SIDE, SIDE, C)
        return jnp.pad(grid, ((0, 0), (0, 0), (0, WIDE - SIDE), (0, 0))).reshape(-1, ROWS, C)

    mine = lax.dynamic_slice_in_dim(section_input[:, 0], core * micro, micro, 0)
    x = widened(mine)
    flags = [(plane == s).astype(jnp.int32).reshape(1) for s in range(planes)]
    flips = flip_all(weights)
    parts = [x[m : m + 1] for m in range(micro)]
    mine_at, other_at = core.astype(jnp.uint32), (1 - core).astype(jnp.uint32)
    class_ids = class_offsets[0] + jnp.arange(class_centers.shape[0], dtype=jnp.int32)
    held, vec, pool_compact, embed_ready = load_weights(
        core.reshape(1), weights, own_vec, peer_vec, depthwise, embed_weight, (*parts, class_ids, *flags, mine_at.reshape(1), other_at.reshape(1))
    )
    saved = {}
    for s in range(planes):
        for m in range(micro):
            parts[m], saved[s, m] = forward_stage(flags[s], parts[m], held, vec)
            if s < planes - 1:
                parts[m] = lax.ppermute(parts[m], "section", [(2 * s + c, 2 * s + 2 + c) for c in range(2)])
    embedded, sent = pool_and_embed(parts, pool_compact, embed_ready, shards)
    width = embedded.shape[-1]
    embedded, depthwise, embed_weight, labels = lax.optimization_barrier(
        (embedded, depthwise, embed_weight, labels)
    )
    pool_weight = widened(depthwise)[0].astype(jnp.float32)

    def my_labels():
        return lax.dynamic_slice_in_dim(labels, core * micro, micro, 0).T.reshape(-1, 1)

    def label_rows():
        centres_unit = unit_scale(class_centers.astype(jnp.float32))[0].astype(jnp.bfloat16)
        rows = jnp.dot(
            (my_labels() == class_ids[None, :]).astype(jnp.bfloat16),
            centres_unit,
            preferred_element_type=jnp.float32,
        ).astype(jnp.bfloat16)
        rows = lax.all_to_all(rows.reshape(shards, micro, width), "shard", 0, 0, tiled=True)
        return jnp.sum(rows.astype(jnp.float32), axis=0).astype(jnp.bfloat16)

    chosen = lax.cond(plane == 0, label_rows, lambda: jnp.zeros((micro, width), jnp.bfloat16))
    chosen = lax.ppermute(chosen, "section", [(c, sections - 2 + c) for c in range(2)])
    unit_half = lax.all_to_all(sent, "shard", 0, 0, tiled=True).reshape(shards * micro, width)
    scale = unit_scale(class_centers.astype(jnp.float32))[2].reshape(1, -1)
    sums = class_sums(unit_half, class_centers, scale, my_labels(), class_ids[None, :], flips)
    sums = lax.all_to_all(sums.reshape(shards, micro, -1), "shard", 0, 0, tiled=True)
    sums = jnp.sum(sums.astype(jnp.float32), axis=0)
    g, flips, zbuf = tail(
        jnp.stack([core, plane]), sums, chosen, embedded, embed_weight, pool_weight, flips,
        [saved[s, m] for s in range(planes) for m in range(micro)],
    )
    parts = [g[m : m + 1] for m in range(micro)]
    stores = [jnp.zeros((2, ROWS, C), jnp.bfloat16) for m in range(micro)]
    for s in reversed(range(planes)):
        for m in range(micro):
            parts[m], stores[m] = backward_stage(m, s == 0, flags[s], parts[m], flips, vec, zbuf, stores[m])
            if s > 0:
                parts[m] = lax.ppermute(parts[m], "section", [(2 * s + c, 2 * s - 2 + c) for c in range(2)])
    store = jnp.stack(stores, axis=1)

    def narrowed(rows):
        return rows.reshape(-1, SIDE, WIDE, C)[:, :, :SIDE].reshape(-1, SIDE * SIDE, C)

    kept = narrowed(lax.dynamic_index_in_dim(store, mine_at, 0, keepdims=False))
    given = narrowed(lax.dynamic_index_in_dim(store, other_at, 0, keepdims=False))
    taken = lax.ppermute(given, "section", swap)
    first = jnp.where(mine_at == 0, kept, taken)
    second = jnp.where(mine_at == 0, taken, kept)
    return jnp.concatenate([first, second], axis=0)[None, :, None]


def solution(mesh):
    placed = (
        P(None, "shard", None, None),
        P("section", None, None),
        P("section", None, None),
        P("section", None),
        P("section", None),
        P("section", None),
        P(),
        P(),
        P("shard", None),
        P(),
        P("shard"),
    )
    return jax.shard_map(
        on_device,
        mesh=mesh,
        in_specs=placed,
        out_specs=P("section", None, "shard", None, None),
        check_vma=False,
    )
```

```python
import functools
import math

import jax
import jax.numpy as jnp
from jax import lax
from jax.experimental import pallas as pl
from jax.experimental.pallas import tpu as pltpu
from jax.sharding import PartitionSpec as P


SIDE = 14
WIDE = 16
ROWS = SIDE * WIDE
C = 256

margin_value = 0.4
scale_value = 64.0
tiny_value = 1e-06

VM = pl.BlockSpec(memory_space=pltpu.VMEM)
AN = pl.BlockSpec(memory_space=pl.ANY)
HB = pl.BlockSpec(memory_space=pltpu.HBM)
SM = pl.BlockSpec(memory_space=pltpu.SMEM)
LIMIT = 20 * 1024 * 1024


def keep_columns(rows):
    return (lax.broadcasted_iota(jnp.int32, (rows, C), 0) % WIDE) < SIDE


HALF = ROWS // 2


def build(value, cols, base):
    rows = value.shape[0]
    parts = (pltpu.roll(value, 1, 0), value, pltpu.roll(value, rows - 1, 0))
    for place, part in enumerate(parts):
        cols[WIDE + base : WIDE + base + rows, place * C : (place + 1) * C] = part.astype(jnp.bfloat16)


def conv(cols, weights, base):
    acc = None
    for step in range(3):
        part = jnp.dot(
            cols[base + WIDE * step : base + WIDE * step + HALF, :],
            weights[step * 3 * C : (step + 1) * 3 * C, :],
            preferred_element_type=jnp.float32,
        )
        acc = part if acc is None else acc + part
    return acc


def clear_border(cols):
    for i in range(2):
        cols[i, 0:WIDE, :] = jnp.zeros((WIDE, 3 * C), jnp.bfloat16)
        cols[i, WIDE + ROWS :, :] = jnp.zeros((WIDE, 3 * C), jnp.bfloat16)


HALVES = tuple(slice(h * HALF, (h + 1) * HALF) for h in range(2))


def start_unit(core, u, own, peer, held, sems):
    @pl.when(core == u)
    def _():
        for k, source in enumerate(own):
            pltpu.make_async_copy(source, held.at[u, k], sems.at[k]).start()

    @pl.when(core != u)
    def _():
        for k, source in enumerate(peer):
            pltpu.make_async_copy(source, held.at[u, k], sems.at[k]).start()


def wait_unit(u, own, held, sems):
    for k, source in enumerate(own):
        pltpu.make_async_copy(source, held.at[u, k], sems.at[k]).wait()


def load_body(flag, own1, own2, peer1, peer2, own_vec, peer_vec, pool, embed, *rest):
    held, vec, pool_out, embed_out, sems, more = rest[-6:]
    core = flag[0]
    start_unit(core, 0, (own1, own2), (peer1, peer2), held, sems)
    copies = [
        pltpu.make_async_copy(pool, pool_out, more.at[0]),
        pltpu.make_async_copy(embed, embed_out, more.at[1]),
    ]
    for copy in copies:
        copy.start()
    vec[core] = own_vec[...]
    vec[1 - core] = peer_vec[...]
    wait_unit(0, (own1, own2), held, sems)
    for copy in copies:
        copy.wait()


def pool_body(first, second, pool_ref, embed_ref, embedded_ref, sent_ref):
    pooled = []
    for image in (first, second):
        total = jnp.zeros((SIDE, C), jnp.float32)
        for i in range(SIDE):
            rows = image[0, WIDE * i : WIDE * i + SIDE, :].astype(jnp.float32)
            total += rows * pool_ref[SIDE * i : SIDE * i + SIDE, :].astype(jnp.float32)
        pooled.append(jnp.sum(total, axis=0, keepdims=True))
    pooled = jnp.concatenate(pooled, axis=0).astype(jnp.bfloat16)
    embedded = jnp.dot(pooled, embed_ref[...], preferred_element_type=jnp.float32)
    embedded_ref[...] = embedded
    normed = unit_scale(embedded)[0].astype(jnp.bfloat16)
    sent_ref[...] = jnp.broadcast_to(normed[None], sent_ref.shape)


def pool_and_embed(parts, pool, embed, shards):
    width = embed.shape[1]
    return pl.pallas_call(
        pool_body,
        in_specs=[VM] * 4,
        out_specs=[VM, VM],
        out_shape=[
            jax.ShapeDtypeStruct((2, width), jnp.float32),
            jax.ShapeDtypeStruct((shards, 2, width), jnp.bfloat16),
        ],
        compiler_params=pltpu.CompilerParams(vmem_limit_bytes=STAGE_LIMIT),
        cost_estimate=pl.CostEstimate(flops=100_000_000, bytes_accessed=1_000_000, transcendentals=0),
        name="pool_and_embed",
    )(*parts, pool, embed)


def head_body(unit_ref, centres_ref, scale_ref, labels_ref, ids_ref, *rest):
    out_ref = rest[-1]
    faces = unit_ref.shape[0]
    width = centres_ref.shape[1]
    centres = centres_ref[...]
    scale = scale_ref[...]
    cosines = lax.dot_general(
        unit_ref[...], centres, (((1,), (1,)), ((), ())), preferred_element_type=jnp.float32
    )
    hits = (labels_ref[...] == ids_ref[...]).astype(jnp.float32)
    weights = jnp.exp(scale_value * (cosines * scale - margin_value * hits))
    totals = jnp.sum(weights, axis=1, keepdims=True)
    weighted = jnp.dot(
        (weights * scale).astype(jnp.bfloat16), centres, preferred_element_type=jnp.float32
    )
    out_ref[:, :width] = weighted.astype(jnp.bfloat16)
    out_ref[:, width:] = jnp.broadcast_to(totals, (faces, 128)).astype(jnp.bfloat16)


def class_sums(unit_half, centres, scale, labels, ids, after):
    faces, width = unit_half.shape
    return pl.pallas_call(
        head_body,
        in_specs=[VM] * 5 + [AN] * len(after),
        out_specs=VM,
        out_shape=jax.ShapeDtypeStruct((faces, width + 128), jnp.bfloat16),
        compiler_params=pltpu.CompilerParams(vmem_limit_bytes=STAGE_LIMIT),
        cost_estimate=pl.CostEstimate(flops=450_000_000, bytes_accessed=2_000_000, transcendentals=220_000),
        name="class_sums",
    )(unit_half, centres, scale, labels, ids, *in_hbm(*after))


def forward_body(first, flag, x_ref, held_in, vec_ref, *rest):
    if first:
        own, peer, held, sems = rest[0:2], rest[2:4], rest[4], rest[-1]
        rest = rest[5:-1]
        start_unit(flag[1], 1, own, peer, held, sems)
    else:
        held = held_in
    out_ref, z_ref, cols, run, zed, zsem = rest

    @pl.when(flag[0] == 1)
    def _():
        clear_border(cols)
        keep = keep_columns(HALF)
        run[...] = x_ref[0].astype(jnp.float32)

        def one(u, carry):
            vec = vec_ref[u]
            for h in HALVES:
                build(run[h], cols.at[0], h.start)
            if first:
                pl.when(u == 1)(lambda: wait_unit(1, own, held, sems))
            for h in HALVES:
                pre = conv(cols.at[0], held.at[u, 0], h.start) * vec[0:1] + vec[1:2]
                zed[u, h] = pre.astype(jnp.bfloat16)
                leak = vec[2:3]
                rest = jnp.log(1.0 + jnp.exp(-4.0 * jnp.abs(pre)))
                active = pre * jnp.where(pre < 0.0, leak, 1.0) + (0.25 * (1.0 - leak)) * rest
                build(jnp.where(keep, active, 0.0), cols.at[1], h.start)
            pltpu.make_async_copy(zed.at[u], z_ref.at[u], zsem.at[u]).start()
            for h in HALVES:
                result = run[h] + conv(cols.at[1], held.at[u, 1], h.start)
                result = jnp.where(keep, result, 0.0).astype(jnp.bfloat16)
                run[h] = result.astype(jnp.float32)
            return carry

        lax.fori_loop(0, 2, one, 0)
        out_ref[0] = run[...].astype(jnp.bfloat16)
        for u in range(2):
            pltpu.make_async_copy(zed.at[u], z_ref.at[u], zsem.at[u]).wait()

    if first:

        @pl.when(flag[0] != 1)
        def _():
            wait_unit(1, own, held, sems)


def backward_body(image, first, flag, g_ref, held_in, vec_ref, z_ref, store_in, *rest):
    if first:
        own, peer, held, sems = rest[0:2], rest[2:4], rest[4], rest[-1]
        rest = rest[5:-1]
        start_unit(flag[1], 0, own, peer, held, sems)
    else:
        held = held_in
    store, cols, run = rest[-3:]

    @pl.when(flag[0] == 1)
    def _():
        clear_border(cols)
        keep = keep_columns(HALF)
        run[...] = g_ref[0].astype(jnp.float32)

        def one(step, carry):
            u = 1 - step
            vec = vec_ref[u]
            half = 0.5 * vec[0:1]
            base = half * (1.0 + vec[2:3])
            gain = half * (1.0 - vec[2:3])
            for h in HALVES:
                build(run[h], cols.at[0], h.start)
            if first:
                pl.when(u == 0)(lambda: wait_unit(0, own, held, sems))
            for h in HALVES:
                slope = base + gain * jnp.tanh(2.0 * z_ref[image, u, h].astype(jnp.float32))
                hidden = conv(cols.at[0], held.at[u, 1], h.start) * slope
                build(jnp.where(keep, hidden, 0.0), cols.at[1], h.start)
            for h in HALVES:
                result = run[h] + conv(cols.at[1], held.at[u, 0], h.start)
                result = jnp.where(keep, result, 0.0).astype(jnp.bfloat16)
                run[h] = result.astype(jnp.float32)
                store[u, h] = result
            return carry

        lax.fori_loop(0, 2, one, 0)
        if len(rest) == 4:
            rest[0][0] = run[...].astype(jnp.bfloat16)

    if first:

        @pl.when(flag[0] != 1)
        def _():
            wait_unit(0, own, held, sems)


def tail_body(
    flag, sums_ref, chosen_ref, embedded_ref, embed_ref, pool_ref, own1, own2, peer1, peer2, *rest
):
    saved, (first_g, second_g, held, zbuf, sems, zsems) = rest[:-6], rest[-6:]
    images = zbuf.shape[0]
    core, plane = flag[0], flag[1]
    start_unit(core, 1, (own1, own2), (peer1, peer2), held, sems)
    for s in range(len(saved) // images):

        @pl.when(plane == s)
        def _():
            for m in range(images):
                pltpu.make_async_copy(saved[s * images + m], zbuf.at[m], zsems.at[m]).start()

    embedded = embedded_ref[...]
    width = embedded.shape[1]
    squares = jnp.sum(embedded * embedded, axis=1, keepdims=True) / width
    factor = lax.rsqrt(squares + tiny_value) / math.sqrt(width)
    total = sums_ref[:, width : width + 1]
    grad_unit = scale_value * (sums_ref[:, :width] / total - chosen_ref[...].astype(jnp.float32))
    inner = jnp.sum(embedded * grad_unit, axis=1, keepdims=True)
    grad_embed = factor * (grad_unit - embedded * inner / (width * (squares + tiny_value)))
    grad_pooled = lax.dot_general(
        grad_embed.astype(jnp.bfloat16),
        embed_ref[...],
        (((1,), (1,)), ((), ())),
        preferred_element_type=jnp.float32,
    )
    for m, g_ref in enumerate((first_g, second_g)):
        g_ref[0] = (grad_pooled[m : m + 1] * pool_ref[...]).astype(jnp.bfloat16)
    wait_unit(1, (own1, own2), held, sems)
    for m in range(images):
        pltpu.make_async_copy(saved[m], zbuf.at[m], zsems.at[m]).wait()


def tail(flag, sums, chosen, embedded, embed_weight, pool_weight, weights, saved):
    images = sums.shape[0]
    return pl.pallas_call(
        tail_body,
        in_specs=[SM, VM, VM, VM, VM, VM] + [HB] * (len(weights) + len(saved)),
        out_specs=[VM] * 4,
        out_shape=[
            jax.ShapeDtypeStruct((1, ROWS, C), jnp.bfloat16),
            jax.ShapeDtypeStruct((1, ROWS, C), jnp.bfloat16),
            jax.ShapeDtypeStruct((2, 2, *weights[0].shape), weights[0].dtype),
            jax.ShapeDtypeStruct((images, 2, ROWS, C), jnp.bfloat16),
        ],
        scratch_shapes=[pltpu.SemaphoreType.DMA((2,)), pltpu.SemaphoreType.DMA((images,))],
        compiler_params=pltpu.CompilerParams(vmem_limit_bytes=STAGE_LIMIT),
        cost_estimate=pl.CostEstimate(flops=300_000_000, bytes_accessed=9_000_000, transcendentals=0),
        name="tail",
    )(flag, sums, chosen, embedded, embed_weight, pool_weight, *in_hbm(*weights), *in_hbm(*saved))


def in_hbm(*arrays):
    return [pltpu.with_memory_space_constraint(a, pltpu.HBM) for a in arrays]


CONV_COST = pl.CostEstimate(flops=4 * 2 * 224 * 2304 * 256, bytes_accessed=6_000_000, transcendentals=250_000)
STAGE_LIMIT = 8 * 1024 * 1024
STAGE_SCRATCH = [
    pltpu.VMEM((2, ROWS + 2 * WIDE, 3 * C), jnp.bfloat16),
    pltpu.VMEM((ROWS, C), jnp.float32),
    pltpu.VMEM((2, ROWS, C), jnp.bfloat16),
    pltpu.SemaphoreType.DMA((2,)),
]


def load_weights(core, weights, own_vec, peer_vec, pool, embed, before):
    return pl.pallas_call(
        load_body,
        in_specs=[SM, HB, HB, AN, AN, VM, VM, HB, HB] + [AN] * len(before),
        out_specs=[VM] * 4,
        out_shape=[
            jax.ShapeDtypeStruct((2, 2, *weights[0].shape), weights[0].dtype),
            jax.ShapeDtypeStruct((2, *own_vec.shape), own_vec.dtype),
            jax.ShapeDtypeStruct(pool.shape, pool.dtype),
            jax.ShapeDtypeStruct(embed.shape, embed.dtype),
        ],
        scratch_shapes=[pltpu.SemaphoreType.DMA((2,)), pltpu.SemaphoreType.DMA((2,))],
        compiler_params=pltpu.CompilerParams(vmem_limit_bytes=STAGE_LIMIT),
        cost_estimate=pl.CostEstimate(flops=300_000_000, bytes_accessed=9_000_000, transcendentals=0),
        name="load_weights",
    )(core, *in_hbm(*weights[:2]), *weights[2:], own_vec, peer_vec, *in_hbm(pool, embed), *before)


def forward_stage(flag, x, held, vec, weights=()):
    first = len(weights) > 0
    outs = pl.pallas_call(
        functools.partial(forward_body, first),
        in_specs=[SM, VM, VM, VM] + [HB] * len(weights),
        out_specs=[VM] * first + [VM, HB],
        out_shape=[jax.ShapeDtypeStruct(held.shape, held.dtype)] * first
        + [
            jax.ShapeDtypeStruct(x.shape, jnp.bfloat16),
            pltpu.HBM((2, ROWS, C), jnp.bfloat16),
        ],
        scratch_shapes=STAGE_SCRATCH + [pltpu.SemaphoreType.DMA((2,))] * first,
        input_output_aliases={2: 0} if first else {},
        compiler_params=pltpu.CompilerParams(vmem_limit_bytes=STAGE_LIMIT),
        cost_estimate=CONV_COST,
        name="forward_stage",
    )(flag, x, held, vec, *in_hbm(*weights))
    return (outs[0] if first else held), outs[-2], outs[-1]


def backward_stage(image, last, flag, g, held, vec, z, store, weights=()):
    first = len(weights) > 0
    shapes = [jax.ShapeDtypeStruct(held.shape, held.dtype)] * first
    shapes += [] if last else [jax.ShapeDtypeStruct(g.shape, jnp.bfloat16)]
    shapes += [jax.ShapeDtypeStruct(store.shape, store.dtype)]
    aliases = {5: len(shapes) - 1}
    if first:
        aliases[2] = 0
    outs = pl.pallas_call(
        functools.partial(backward_body, image, first),
        in_specs=[SM, VM, VM, VM, VM, VM] + [HB] * len(weights),
        out_specs=[VM] * len(shapes),
        out_shape=shapes,
        scratch_shapes=STAGE_SCRATCH[:2] + [pltpu.SemaphoreType.DMA((2,))] * first,
        input_output_aliases=aliases,
        compiler_params=pltpu.CompilerParams(vmem_limit_bytes=STAGE_LIMIT),
        cost_estimate=CONV_COST,
        name="backward_stage",
    )(flag, g, held, vec, z, store, *in_hbm(*weights))
    return (outs[0] if first else held), (None if last else outs[-2]), outs[-1]


def flip_body(*refs):
    eye = (
        lax.broadcasted_iota(jnp.int32, (C, C), 0) == lax.broadcasted_iota(jnp.int32, (C, C), 1)
    ).astype(jnp.float32).astype(jnp.bfloat16)
    half = len(refs) // 2
    for source, target in zip(refs[:half], refs[half:]):
        turned = lax.dot_general(
            eye, source[...], (((1,), (1,)), ((), ())), preferred_element_type=jnp.float32
        )
        target[...] = turned.astype(jnp.bfloat16)


def flip_all(weights):
    count = len(weights)
    return pl.pallas_call(
        flip_body,
        grid=(9,),
        in_specs=[pl.BlockSpec((C, C), lambda t: (t, 0))] * count,
        out_specs=[pl.BlockSpec((C, C), lambda t: (8 - t, 0))] * count,
        out_shape=[pltpu.HBM(w.shape, w.dtype) for w in weights],
        compiler_params=pltpu.CompilerParams(vmem_limit_bytes=LIMIT),
        cost_estimate=pl.CostEstimate(flops=36 * 2 * 256**3, bytes_accessed=9_000_000, transcendentals=0),
        name="flip_all",
    )(*in_hbm(*weights))


def unit_scale(values):
    squares = jnp.mean(values * values, axis=-1, keepdims=True)
    factor = lax.rsqrt(squares + tiny_value) / math.sqrt(values.shape[-1])
    return (values * factor, squares, factor)


def on_device(
    section_input,
    conv_one,
    conv_two,
    unit_gain,
    offset_bias,
    leak_slope,
    depthwise,
    embed_weight,
    class_centers,
    labels,
    class_offsets,
):
    sections = lax.axis_size("section")
    shards = lax.axis_size("shard")
    planes = sections // 2
    section_index = lax.axis_index("section")
    plane = section_index // 2
    core = section_index % 2
    swap = [(s, s ^ 1) for s in range(sections)]

    own = (conv_one[0], conv_two[0])
    peer = tuple(lax.ppermute(w, "section", swap) for w in own)
    weights = (*own, *peer)
    own_vec = jnp.concatenate([unit_gain, offset_bias, leak_slope], axis=0)
    peer_vec = lax.ppermute(own_vec, "section", swap)
    micro = section_input.shape[0] // 2

    def widened(rows):
        grid = rows.reshape(-1, SIDE, SIDE, C)
        return jnp.pad(grid, ((0, 0), (0, 0), (0, WIDE - SIDE), (0, 0))).reshape(-1, ROWS, C)

    mine = lax.dynamic_slice_in_dim(section_input[:, 0], core * micro, micro, 0)
    x = widened(mine)
    flags = [(plane == s).astype(jnp.int32).reshape(1) for s in range(planes)]
    flips = flip_all(weights)
    parts = [x[m : m + 1] for m in range(micro)]
    mine_at, other_at = core.astype(jnp.uint32), (1 - core).astype(jnp.uint32)
    opening = jnp.stack([flags[0][0], core])
    closing = jnp.stack([flags[planes - 1][0], core])
    class_ids = class_offsets[0] + jnp.arange(class_centers.shape[0], dtype=jnp.int32)
    held, vec, pool_compact, embed_ready = load_weights(
        core.reshape(1), weights, own_vec, peer_vec, depthwise, embed_weight, (*parts, class_ids, *flags, opening, closing, mine_at.reshape(1), other_at.reshape(1))
    )
    saved = {}
    for s in range(planes):
        for m in reversed(range(micro)):
            lead = s == 0 and m == micro - 1
            held, parts[m], saved[s, m] = forward_stage(
                opening if lead else flags[s], parts[m], held, vec, weights if lead else ()
            )
            if s < planes - 1:
                pairs = [(2 * s + c, 2 * s + 2 + c) for c in range(2)]
                parts[m] = lax.ppermute(parts[m], "section", pairs)
    embedded, sent = pool_and_embed(parts, pool_compact, embed_ready, shards)
    width = embedded.shape[-1]
    embedded, depthwise, embed_weight, labels = lax.optimization_barrier(
        (embedded, depthwise, embed_weight, labels)
    )
    pool_weight = widened(depthwise)[0].astype(jnp.float32)

    def my_labels():
        return lax.dynamic_slice_in_dim(labels, core * micro, micro, 0).T.reshape(-1, 1)

    def label_rows():
        centres_unit = unit_scale(class_centers.astype(jnp.float32))[0].astype(jnp.bfloat16)
        rows = jnp.dot(
            (my_labels() == class_ids[None, :]).astype(jnp.bfloat16),
            centres_unit,
            preferred_element_type=jnp.float32,
        ).astype(jnp.bfloat16)
        rows = lax.all_to_all(rows.reshape(shards, micro, width), "shard", 0, 0, tiled=True)
        return jnp.sum(rows.astype(jnp.float32), axis=0).astype(jnp.bfloat16)

    chosen = lax.cond(plane == 0, label_rows, lambda: jnp.zeros((micro, width), jnp.bfloat16))
    chosen = lax.ppermute(chosen, "section", [(c, sections - 2 + c) for c in range(2)])
    unit_half = lax.all_to_all(sent, "shard", 0, 0, tiled=True).reshape(shards * micro, width)
    scale = unit_scale(class_centers.astype(jnp.float32))[2].reshape(1, -1)
    sums = class_sums(unit_half, class_centers, scale, my_labels(), class_ids[None, :], flips)
    sums = lax.all_to_all(sums.reshape(shards, micro, -1), "shard", 0, 0, tiled=True)
    sums = jnp.sum(sums.astype(jnp.float32), axis=0)
    *parts, held, zbuf = tail(
        jnp.stack([core, plane]), sums, chosen, embedded, embed_weight, pool_weight, flips,
        [saved[s, m] for s in range(planes) for m in range(micro)],
    )
    stores = [jnp.zeros((2, ROWS, C), jnp.bfloat16) for _ in range(micro)]
    for s in reversed(range(planes)):
        for m in reversed(range(micro)):
            lead = s == planes - 1 and m == micro - 1
            held, parts[m], stores[m] = backward_stage(
                m, s == 0, closing if lead else flags[s], parts[m], held, vec, zbuf, stores[m],
                flips if lead else (),
            )
            if s > 0:
                pairs = [(2 * s + c, 2 * s - 2 + c) for c in range(2)]
                parts[m] = lax.ppermute(parts[m], "section", pairs)
    store = jnp.stack(stores, axis=1)

    def narrowed(rows):
        return rows.reshape(-1, SIDE, WIDE, C)[:, :, :SIDE].reshape(-1, SIDE * SIDE, C)

    kept = narrowed(lax.dynamic_index_in_dim(store, mine_at, 0, keepdims=False))
    given = narrowed(lax.dynamic_index_in_dim(store, other_at, 0, keepdims=False))
    taken = lax.ppermute(given, "section", swap)
    first = jnp.where(mine_at == 0, kept, taken)
    second = jnp.where(mine_at == 0, taken, kept)
    return jnp.concatenate([first, second], axis=0)[None, :, None]


def solution(mesh):
    placed = (
        P(None, "shard", None, None),
        P("section", None, None),
        P("section", None, None),
        P("section", None),
        P("section", None),
        P("section", None),
        P(),
        P(),
        P("shard", None),
        P(),
        P("shard"),
    )
    return jax.shard_map(
        on_device,
        mesh=mesh,
        in_specs=placed,
        out_specs=P("section", None, "shard", None, None),
        check_vma=False,
    )
```

```python
import functools
import math

import jax
import jax.numpy as jnp
from jax import lax
from jax.experimental import pallas as pl
from jax.experimental.pallas import tpu as pltpu
from jax.sharding import PartitionSpec as P


SIDE = 14
WIDE = 16
ROWS = SIDE * WIDE
C = 256

margin_value = 0.4
scale_value = 64.0
tiny_value = 1e-06

VM = pl.BlockSpec(memory_space=pltpu.VMEM)
AN = pl.BlockSpec(memory_space=pl.ANY)
HB = pl.BlockSpec(memory_space=pltpu.HBM)
SM = pl.BlockSpec(memory_space=pltpu.SMEM)
LIMIT = 20 * 1024 * 1024


def keep_columns(rows):
    return (lax.broadcasted_iota(jnp.int32, (rows, C), 0) % WIDE) < SIDE


HALF = ROWS // 2


def build(value, cols, base):
    rows = value.shape[0]
    parts = (pltpu.roll(value, 1, 0), value, pltpu.roll(value, rows - 1, 0))
    for place, part in enumerate(parts):
        cols[WIDE + base : WIDE + base + rows, place * C : (place + 1) * C] = part.astype(jnp.bfloat16)


def conv(cols, weights, base):
    acc = None
    for step in range(3):
        part = jnp.dot(
            cols[base + WIDE * step : base + WIDE * step + HALF, :],
            weights[step * 3 * C : (step + 1) * 3 * C, :],
            preferred_element_type=jnp.float32,
        )
        acc = part if acc is None else acc + part
    return acc


def spread(rows_ref, run):
    for i in range(SIDE):
        run[WIDE * i : WIDE * i + SIDE, :] = rows_ref[SIDE * i : SIDE * i + SIDE, :].astype(jnp.float32)
        run[WIDE * i + SIDE : WIDE * (i + 1), :] = jnp.zeros((WIDE - SIDE, C), jnp.float32)


def gather_rows(run, rows_ref):
    for i in range(SIDE):
        rows_ref[SIDE * i : SIDE * i + SIDE, :] = run[WIDE * i : WIDE * i + SIDE, :].astype(jnp.bfloat16)


def clear_border(cols):
    for i in range(2):
        cols[i, 0:WIDE, :] = jnp.zeros((WIDE, 3 * C), jnp.bfloat16)
        cols[i, WIDE + ROWS :, :] = jnp.zeros((WIDE, 3 * C), jnp.bfloat16)


HALVES = tuple(slice(h * HALF, (h + 1) * HALF) for h in range(2))


def load_body(flag, own1, own2, peer1, peer2, own_vec, peer_vec, pool, embed, *rest):
    held, vec, pool_out, embed_out, sems, more = rest[-6:]
    core = flag[0]
    copies = [
        pltpu.make_async_copy(source, held.at[place, k], sems.at[side, k])
        for side, place, pair in ((0, core, (own1, own2)), (1, 1 - core, (peer1, peer2)))
        for k, source in enumerate(pair)
    ] + [
        pltpu.make_async_copy(pool, pool_out, more.at[0]),
        pltpu.make_async_copy(embed, embed_out, more.at[1]),
    ]
    for copy in copies:
        copy.start()
    vec[core] = own_vec[...]
    vec[1 - core] = peer_vec[...]
    for copy in copies:
        copy.wait()


def pool_body(first, second, pool_ref, embed_ref, embedded_ref, sent_ref):
    weight = pool_ref[...].astype(jnp.float32)
    pooled = [
        jnp.sum(image[0].astype(jnp.float32) * weight, axis=0, keepdims=True) for image in (first, second)
    ]
    pooled = jnp.concatenate(pooled, axis=0).astype(jnp.bfloat16)
    embedded = jnp.dot(pooled, embed_ref[...], preferred_element_type=jnp.float32)
    embedded_ref[...] = embedded
    normed = unit_scale(embedded)[0].astype(jnp.bfloat16)
    sent_ref[...] = jnp.broadcast_to(normed[None], sent_ref.shape)


def pool_and_embed(parts, pool, embed, shards):
    width = embed.shape[1]
    return pl.pallas_call(
        pool_body,
        in_specs=[VM] * 4,
        out_specs=[VM, VM],
        out_shape=[
            jax.ShapeDtypeStruct((2, width), jnp.float32),
            jax.ShapeDtypeStruct((shards, 2, width), jnp.bfloat16),
        ],
        compiler_params=pltpu.CompilerParams(vmem_limit_bytes=STAGE_LIMIT),
        cost_estimate=pl.CostEstimate(flops=100_000_000, bytes_accessed=1_000_000, transcendentals=0),
        name="pool_and_embed",
    )(*parts, pool, embed)


def head_body(unit_ref, centres_ref, scale_ref, labels_ref, ids_ref, *rest):
    out_ref = rest[-1]
    faces = unit_ref.shape[0]
    width = centres_ref.shape[1]
    centres = centres_ref[...]
    scale = scale_ref[...]
    cosines = lax.dot_general(
        unit_ref[...], centres, (((1,), (1,)), ((), ())), preferred_element_type=jnp.float32
    )
    hits = (labels_ref[...] == ids_ref[...]).astype(jnp.float32)
    weights = jnp.exp(scale_value * (cosines * scale - margin_value * hits))
    totals = jnp.sum(weights, axis=1, keepdims=True)
    weighted = jnp.dot(
        (weights * scale).astype(jnp.bfloat16), centres, preferred_element_type=jnp.float32
    )
    out_ref[:, :width] = weighted.astype(jnp.bfloat16)
    out_ref[:, width:] = jnp.broadcast_to(totals, (faces, 128)).astype(jnp.bfloat16)


def class_sums(unit_half, centres, scale, labels, ids, after):
    faces, width = unit_half.shape
    return pl.pallas_call(
        head_body,
        in_specs=[VM] * 5 + [AN] * len(after),
        out_specs=VM,
        out_shape=jax.ShapeDtypeStruct((faces, width + 128), jnp.bfloat16),
        compiler_params=pltpu.CompilerParams(vmem_limit_bytes=STAGE_LIMIT),
        cost_estimate=pl.CostEstimate(flops=450_000_000, bytes_accessed=2_000_000, transcendentals=220_000),
        name="class_sums",
    )(unit_half, centres, scale, labels, ids, *in_hbm(*after))


def forward_body(flag, x_ref, held, vec_ref, out_ref, z_ref, cols, run, zed, zsem):
    @pl.when(flag[0] == 1)
    def _():
        clear_border(cols)
        keep = keep_columns(HALF)
        spread(x_ref.at[0], run)

        def one(u, carry):
            vec = vec_ref[u]
            for h in HALVES:
                build(run[h], cols.at[0], h.start)
            for h in HALVES:
                pre = conv(cols.at[0], held.at[u, 0], h.start) * vec[0:1] + vec[1:2]
                zed[u, h] = pre.astype(jnp.bfloat16)
                leak = vec[2:3]
                rest = jnp.log(1.0 + jnp.exp(-4.0 * jnp.abs(pre)))
                active = pre * jnp.where(pre < 0.0, leak, 1.0) + (0.25 * (1.0 - leak)) * rest
                build(jnp.where(keep, active, 0.0), cols.at[1], h.start)
                part = pl.ds(h.start, HALF)
                pltpu.make_async_copy(
                    zed.at[u, part], z_ref.at[u, part], zsem.at[u, h.start // HALF]
                ).start()
            for h in HALVES:
                result = run[h] + conv(cols.at[1], held.at[u, 1], h.start)
                result = jnp.where(keep, result, 0.0).astype(jnp.bfloat16)
                run[h] = result.astype(jnp.float32)
            return carry

        lax.fori_loop(0, 2, one, 0)
        gather_rows(run, out_ref.at[0])
        for u in range(2):
            for h in HALVES:
                part = pl.ds(h.start, HALF)
                pltpu.make_async_copy(
                    zed.at[u, part], z_ref.at[u, part], zsem.at[u, h.start // HALF]
                ).wait()


def backward_body(image, flag, g_ref, held, vec_ref, z_ref, store_in, *rest):
    store, cols, run = rest[-3:]

    @pl.when(flag[0] == 1)
    def _():
        clear_border(cols)
        keep = keep_columns(HALF)
        spread(g_ref.at[0], run)

        def one(step, carry):
            u = 1 - step
            vec = vec_ref[u]
            half = 0.5 * vec[0:1]
            base = half * (1.0 + vec[2:3])
            gain = half * (1.0 - vec[2:3])
            for h in HALVES:
                build(run[h], cols.at[0], h.start)
            for h in HALVES:
                slope = base + gain * jnp.tanh(2.0 * z_ref[image, u, h].astype(jnp.float32))
                hidden = conv(cols.at[0], held.at[u, 1], h.start) * slope
                build(jnp.where(keep, hidden, 0.0), cols.at[1], h.start)
            for h in HALVES:
                result = run[h] + conv(cols.at[1], held.at[u, 0], h.start)
                result = jnp.where(keep, result, 0.0).astype(jnp.bfloat16)
                run[h] = result.astype(jnp.float32)
            gather_rows(run, store.at[u])
            return carry

        lax.fori_loop(0, 2, one, 0)
        if len(rest) == 4:
            gather_rows(run, rest[0].at[0])


def tail_body(
    flag, sums_ref, chosen_ref, embedded_ref, embed_ref, pool_ref, own1, own2, peer1, peer2, *rest
):
    saved, (g_ref, held, zbuf, sems, zsems) = rest[:-5], rest[-5:]
    images = zbuf.shape[0]
    core, plane = flag[0], flag[1]
    copies = [
        pltpu.make_async_copy(source, held.at[place, k], sems.at[side, k])
        for side, place, pair in ((0, core, (own1, own2)), (1, 1 - core, (peer1, peer2)))
        for k, source in enumerate(pair)
    ]
    for copy in copies:
        copy.start()
    for s in range(len(saved) // images):

        @pl.when(plane == s)
        def _():
            for m in range(images):
                pltpu.make_async_copy(saved[s * images + m], zbuf.at[m], zsems.at[m]).start()

    embedded = embedded_ref[...]
    width = embedded.shape[1]
    squares = jnp.sum(embedded * embedded, axis=1, keepdims=True) / width
    factor = lax.rsqrt(squares + tiny_value) / math.sqrt(width)
    total = sums_ref[:, width : width + 1]
    grad_unit = scale_value * (sums_ref[:, :width] / total - chosen_ref[...].astype(jnp.float32))
    inner = jnp.sum(embedded * grad_unit, axis=1, keepdims=True)
    grad_embed = factor * (grad_unit - embedded * inner / (width * (squares + tiny_value)))
    grad_pooled = lax.dot_general(
        grad_embed.astype(jnp.bfloat16),
        embed_ref[...],
        (((1,), (1,)), ((), ())),
        preferred_element_type=jnp.float32,
    )
    for m in range(images):
        g_ref[m] = (grad_pooled[m : m + 1] * pool_ref[...]).astype(jnp.bfloat16)
    for copy in copies:
        copy.wait()
    for m in range(images):
        pltpu.make_async_copy(saved[m], zbuf.at[m], zsems.at[m]).wait()


def tail(flag, sums, chosen, embedded, embed_weight, pool_weight, weights, saved):
    images = sums.shape[0]
    return pl.pallas_call(
        tail_body,
        in_specs=[SM, VM, VM, VM, VM, VM] + [HB] * (len(weights) + len(saved)),
        out_specs=[VM, VM, VM],
        out_shape=[
            jax.ShapeDtypeStruct((images, SIDE * SIDE, C), jnp.bfloat16),
            jax.ShapeDtypeStruct((2, 2, *weights[0].shape), weights[0].dtype),
            jax.ShapeDtypeStruct((images, 2, ROWS, C), jnp.bfloat16),
        ],
        scratch_shapes=[pltpu.SemaphoreType.DMA((2, 2)), pltpu.SemaphoreType.DMA((images,))],
        compiler_params=pltpu.CompilerParams(vmem_limit_bytes=STAGE_LIMIT),
        cost_estimate=pl.CostEstimate(flops=300_000_000, bytes_accessed=9_000_000, transcendentals=0),
        name="tail",
    )(flag, sums, chosen, embedded, embed_weight, pool_weight, *in_hbm(*weights), *in_hbm(*saved))


def in_hbm(*arrays):
    return [pltpu.with_memory_space_constraint(a, pltpu.HBM) for a in arrays]


CONV_COST = pl.CostEstimate(flops=4 * 2 * 224 * 2304 * 256, bytes_accessed=6_000_000, transcendentals=250_000)
STAGE_LIMIT = 8 * 1024 * 1024
STAGE_SCRATCH = [
    pltpu.VMEM((2, ROWS + 2 * WIDE, 3 * C), jnp.bfloat16),
    pltpu.VMEM((ROWS, C), jnp.float32),
    pltpu.VMEM((2, ROWS, C), jnp.bfloat16),
    pltpu.SemaphoreType.DMA((2, 2)),
]


def load_weights(core, weights, own_vec, peer_vec, pool, embed, before):
    return pl.pallas_call(
        load_body,
        in_specs=[SM, HB, HB, AN, AN, VM, VM, HB, HB] + [AN] * len(before),
        out_specs=[VM] * 4,
        out_shape=[
            jax.ShapeDtypeStruct((2, 2, *weights[0].shape), weights[0].dtype),
            jax.ShapeDtypeStruct((2, *own_vec.shape), own_vec.dtype),
            jax.ShapeDtypeStruct(pool.shape, pool.dtype),
            jax.ShapeDtypeStruct(embed.shape, embed.dtype),
        ],
        scratch_shapes=[pltpu.SemaphoreType.DMA((2, 2)), pltpu.SemaphoreType.DMA((2,))],
        compiler_params=pltpu.CompilerParams(vmem_limit_bytes=STAGE_LIMIT),
        cost_estimate=pl.CostEstimate(flops=300_000_000, bytes_accessed=9_000_000, transcendentals=0),
        name="load_weights",
    )(core, *in_hbm(*weights[:2]), *weights[2:], own_vec, peer_vec, *in_hbm(pool, embed), *before)


def forward_stage(flag, x, held, vec):
    return pl.pallas_call(
        forward_body,
        in_specs=[SM, VM, VM, VM],
        out_specs=[VM, HB],
        out_shape=[
            jax.ShapeDtypeStruct(x.shape, jnp.bfloat16),
            pltpu.HBM((2, ROWS, C), jnp.bfloat16),
        ],
        scratch_shapes=STAGE_SCRATCH,
        compiler_params=pltpu.CompilerParams(vmem_limit_bytes=STAGE_LIMIT),
        cost_estimate=CONV_COST,
        name="forward_stage",
    )(flag, x, held, vec)


def backward_stage(image, last, flag, g, held, vec, z, store):
    passed = [] if last else [jax.ShapeDtypeStruct(g.shape, jnp.bfloat16)]
    outs = pl.pallas_call(
        functools.partial(backward_body, image),
        in_specs=[SM, VM, VM, VM, VM, VM],
        out_specs=[VM] * (len(passed) + 1),
        out_shape=passed + [jax.ShapeDtypeStruct(store.shape, store.dtype)],
        scratch_shapes=STAGE_SCRATCH[:2],
        input_output_aliases={5: len(passed)},
        compiler_params=pltpu.CompilerParams(vmem_limit_bytes=STAGE_LIMIT),
        cost_estimate=CONV_COST,
        name="backward_stage",
    )(flag, g, held, vec, z, store)
    return outs[0], outs[-1]


def flip_body(*refs):
    eye = (
        lax.broadcasted_iota(jnp.int32, (C, C), 0) == lax.broadcasted_iota(jnp.int32, (C, C), 1)
    ).astype(jnp.float32).astype(jnp.bfloat16)
    half = len(refs) // 2
    for source, target in zip(refs[:half], refs[half:]):
        turned = lax.dot_general(
            eye, source[...], (((1,), (1,)), ((), ())), preferred_element_type=jnp.float32
        )
        target[...] = turned.astype(jnp.bfloat16)


def flip_all(weights):
    count = len(weights)
    return pl.pallas_call(
        flip_body,
        grid=(9,),
        in_specs=[pl.BlockSpec((C, C), lambda t: (t, 0))] * count,
        out_specs=[pl.BlockSpec((C, C), lambda t: (8 - t, 0))] * count,
        out_shape=[pltpu.HBM(w.shape, w.dtype) for w in weights],
        compiler_params=pltpu.CompilerParams(vmem_limit_bytes=LIMIT),
        cost_estimate=pl.CostEstimate(flops=36 * 2 * 256**3, bytes_accessed=9_000_000, transcendentals=0),
        name="flip_all",
    )(*in_hbm(*weights))


def unit_scale(values):
    squares = jnp.mean(values * values, axis=-1, keepdims=True)
    factor = lax.rsqrt(squares + tiny_value) / math.sqrt(values.shape[-1])
    return (values * factor, squares, factor)


def on_device(
    section_input,
    conv_one,
    conv_two,
    unit_gain,
    offset_bias,
    leak_slope,
    depthwise,
    embed_weight,
    class_centers,
    labels,
    class_offsets,
):
    sections = lax.axis_size("section")
    shards = lax.axis_size("shard")
    planes = sections // 2
    section_index = lax.axis_index("section")
    plane = section_index // 2
    core = section_index % 2
    swap = [(s, s ^ 1) for s in range(sections)]

    own = (conv_one[0], conv_two[0])
    peer = tuple(lax.ppermute(w, "section", swap) for w in own)
    weights = (*own, *peer)
    own_vec = jnp.concatenate([unit_gain, offset_bias, leak_slope], axis=0)
    peer_vec = lax.ppermute(own_vec, "section", swap)
    micro = section_input.shape[0] // 2

    mine = lax.dynamic_slice_in_dim(section_input[:, 0], core * micro, micro, 0)
    x = lax.optimization_barrier(mine)
    flags = [(plane == s).astype(jnp.int32).reshape(1) for s in range(planes)]
    parts = [x[m : m + 1] for m in range(micro)]
    mine_at, other_at = core.astype(jnp.uint32), (1 - core).astype(jnp.uint32)
    class_ids = class_offsets[0] + jnp.arange(class_centers.shape[0], dtype=jnp.int32)
    held, vec, pool_compact, embed_ready = load_weights(
        core.reshape(1), weights, own_vec, peer_vec, depthwise, embed_weight, (*parts, class_ids, *flags, mine_at.reshape(1), other_at.reshape(1))
    )
    saved = {}
    for s in range(planes):
        for m in range(micro):
            parts[m], saved[s, m] = forward_stage(flags[s], parts[m], held, vec)
            if s < planes - 1:
                parts[m] = lax.ppermute(parts[m], "section", [(2 * s + c, 2 * s + 2 + c) for c in range(2)])
    embedded, sent = pool_and_embed(parts, pool_compact, embed_ready, shards)
    width = embedded.shape[-1]
    embedded, depthwise, embed_weight, labels = lax.optimization_barrier(
        (embedded, depthwise, embed_weight, labels)
    )
    pool_weight = depthwise.astype(jnp.float32)

    def my_labels():
        return lax.dynamic_slice_in_dim(labels, core * micro, micro, 0).T.reshape(-1, 1)

    def label_rows():
        centres_unit = unit_scale(class_centers.astype(jnp.float32))[0].astype(jnp.bfloat16)
        rows = jnp.dot(
            (my_labels() == class_ids[None, :]).astype(jnp.bfloat16),
            centres_unit,
            preferred_element_type=jnp.float32,
        ).astype(jnp.bfloat16)
        rows = lax.all_to_all(rows.reshape(shards, micro, width), "shard", 0, 0, tiled=True)
        return jnp.sum(rows.astype(jnp.float32), axis=0).astype(jnp.bfloat16)

    chosen = lax.cond(plane == 0, label_rows, lambda: jnp.zeros((micro, width), jnp.bfloat16))
    chosen = lax.ppermute(chosen, "section", [(c, sections - 2 + c) for c in range(2)])
    flips = flip_all(weights)
    unit_half = lax.all_to_all(sent, "shard", 0, 0, tiled=True).reshape(shards * micro, width)
    scale = unit_scale(class_centers.astype(jnp.float32))[2].reshape(1, -1)
    sums = class_sums(unit_half, class_centers, scale, my_labels(), class_ids[None, :], ())
    sums = lax.all_to_all(sums.reshape(shards, micro, -1), "shard", 0, 0, tiled=True)
    sums = jnp.sum(sums.astype(jnp.float32), axis=0)
    g, flips, zbuf = tail(
        jnp.stack([core, plane]), sums, chosen, embedded, embed_weight, pool_weight, flips,
        [saved[s, m] for s in range(planes) for m in range(micro)],
    )
    parts = [g[m : m + 1] for m in range(micro)]
    stores = [jnp.zeros((2, SIDE * SIDE, C), jnp.bfloat16) for _ in range(micro)]
    for s in reversed(range(planes)):
        for m in range(micro):
            parts[m], stores[m] = backward_stage(m, s == 0, flags[s], parts[m], flips, vec, zbuf, stores[m])
            if s > 0:
                parts[m] = lax.ppermute(parts[m], "section", [(2 * s + c, 2 * s - 2 + c) for c in range(2)])
    store = jnp.stack(stores, axis=1)

    kept = lax.dynamic_index_in_dim(store, mine_at, 0, keepdims=False)
    given = lax.dynamic_index_in_dim(store, other_at, 0, keepdims=False)
    taken = lax.ppermute(given, "section", swap)
    first = jnp.where(mine_at == 0, kept, taken)
    second = jnp.where(mine_at == 0, taken, kept)
    return jnp.concatenate([first, second], axis=0)[None, :, None]


def solution(mesh):
    placed = (
        P(None, "shard", None, None),
        P("section", None, None),
        P("section", None, None),
        P("section", None),
        P("section", None),
        P("section", None),
        P(),
        P(),
        P("shard", None),
        P(),
        P("shard"),
    )
    return jax.shard_map(
        on_device,
        mesh=mesh,
        in_specs=placed,
        out_specs=P("section", None, "shard", None, None),
        check_vma=False,
    )
```
